512 devices in a mesh: blk: 16 (over x_lo, y, core), group: 32 (over x_hi, z).
Axes of the slice: x: 4 (x_hi: 2, x_lo: 2; x = x_hi * 2 + x_lo), y: 4, z: 16, core: 2. Of those that a mesh axis runs over, the one named last changes fastest.
Arguments:
- queries: bfloat16 [512, 16, 128], P(('blk', 'group')), may hold values from -2.5 to 2.5
- query_mask: int32 [512, 16], P(('blk', 'group')), may hold values from 0 to 1, as said below
- positive: int32 [512], P(('blk', 'group')), may hold values from 0 to 1023
- page_vectors: bfloat16 [1024, 128, 128], P(('blk', 'group')), may hold values from -2 to 2
- page_mask: int32 [1024, 128], P(('blk', 'group')), may hold values from 0 to 1, as said below
Outputs:
- grad_queries: float32 [512, 16, 128], P(('blk', 'group'))
- grad_pages: float32 [1024, 128, 128], P(('blk', 'group'))
- mean_loss: float32 [], replicated
The draws below stay inside these ranges and needn't reach their ends.
Inputs may be any that keep to these rules, and one draw needn't show every extreme that they name: `query_mask`: each row holds ones on its first 8 to 16 token slots and zeros after them. `page_mask`: each row holds ones on its first 32 to 128 patch slots and zeros after them.
All inputs are finite; a program needn't handle non-finite values.
Results may differ from the reference program's by a relative error of at most 0.0028.
Values may be sent and summed in bfloat16 or wider, within the bound.
A program may use at most 64 MiB of HBM per device.

```python
import math
import jax
import jax.numpy as jnp
from jax import lax

D = 128
QT = 16
PATCH = 128
Q = 512
PAGES = 1024


def draw_queries(key, part):
    own_key = jax.random.fold_in(key, 11)
    values = jnp.clip(0.36 * jax.random.normal(own_key, (Q, QT, D), jnp.float32), -2.5, 2.5)
    return values.astype(jnp.bfloat16)


def draw_page_vectors(key, part):
    own_key = jax.random.fold_in(key, 13)
    values = jnp.clip(0.36 * jax.random.normal(own_key, (PAGES, PATCH, D), jnp.float32), -2.0, 2.0)
    return values.astype(jnp.bfloat16)


def draw_query_mask(key, part):
    lengths = jax.random.randint(jax.random.fold_in(key, 17), (Q, 1), QT // 2, QT + 1)
    return (jnp.arange(QT, dtype=jnp.int32)[None, :] < lengths).astype(jnp.int32)


def draw_page_mask(key, part):
    lengths = jax.random.randint(jax.random.fold_in(key, 19), (PAGES, 1), PATCH // 4, PATCH + 1)
    return (jnp.arange(PATCH, dtype=jnp.int32)[None, :] < lengths).astype(jnp.int32)


def set_ends(drawn, key, smallest, largest):
    longest = drawn.shape.index(max(drawn.shape))
    spots = []
    for shift in (0, 1):
        where = [jax.random.randint(jax.random.fold_in(key, axis), (), 0, length) for axis, length in enumerate(drawn.shape)]
        where[longest] = (where[longest] + shift) % drawn.shape[longest]
        spots.append(tuple(where))
    return drawn.at[spots[0]].set(smallest).at[spots[1]].set(largest)


def setup_inputs(seed: int = 0) -> dict:
    key_of = jax.random.split(jax.random.key(seed), 6)
    return {
        "queries": draw_queries(jax.random.fold_in(key_of[5], 71), 0),
        "query_mask": draw_query_mask(jax.random.fold_in(key_of[5], 71), 0),
        "positive": set_ends(jax.random.randint(key_of[2], (Q,), 0, PAGES), jax.random.fold_in(key_of[2], 1), 0, PAGES - 1).astype(jnp.int32),
        "page_vectors": draw_page_vectors(jax.random.fold_in(key_of[5], 71), 0),
        "page_mask": draw_page_mask(jax.random.fold_in(key_of[5], 71), 0),
    }


relaxation_scale_factor = 0.5
guarded_floor_entry = -1.0e30


def masked_logits(question_embedding_matrix, lone_document, live_image_embeddings):
    similarity_matrix = jnp.dot(question_embedding_matrix, lone_document.T, preferred_element_type=jnp.float32) / relaxation_scale_factor
    return jnp.where(live_image_embeddings[None, :] > 0, similarity_matrix, guarded_floor_entry)


def reference(queries, query_mask, positive, page_vectors, page_mask):
    question_embedding_matrix = queries.reshape(Q * QT, D).astype(jnp.float32)
    vectors_wide = page_vectors.astype(jnp.float32)
    live_tokens = query_mask.astype(jnp.float32)
    document_region_number = jnp.sum(page_mask.astype(jnp.float32), axis=1)
    page_group = math.gcd(PAGES, 8)
    grouped_pages = vectors_wide.reshape(PAGES // page_group, page_group, PATCH, D)
    grouped_masks = page_mask.reshape(PAGES // page_group, page_group, PATCH)

    def forward(bundle):
        page_block, mask_block = bundle
        found_sums = []
        for number in range(page_group):
            masked = masked_logits(question_embedding_matrix, page_block[number], mask_block[number])
            highest = jnp.max(masked, axis=1, keepdims=True)
            found_sums.append(highest[:, 0] + jnp.log(jnp.sum(jnp.exp(masked - highest), axis=1)))
        return jnp.stack(found_sums)

    logsumexp_results = lax.map(forward, (grouped_pages, grouped_masks))
    linear_accumulated_totals = logsumexp_results.reshape(PAGES, Q, QT)
    softened_supremum = relaxation_scale_factor * (linear_accumulated_totals - jnp.log(document_region_number)[:, None, None])
    scores = jnp.sum(live_tokens[None] * softened_supremum, axis=2).T
    highest = jnp.max(scores, axis=1)
    totals = jnp.sum(jnp.exp(scores - highest[:, None]), axis=1)
    page_lse = highest + jnp.log(totals)
    chosen = positive[:, None] == jnp.arange(PAGES, dtype=jnp.int32)[None, :]
    picked = jnp.sum(jnp.where(chosen, scores, 0.0))
    mean_loss = (jnp.sum(page_lse) - picked) / Q
    coefficient = jnp.exp(scores - page_lse[:, None]) - chosen.astype(jnp.float32)
    factor_scale = (coefficient.T[:, :, None] * live_tokens[None]).reshape(PAGES // page_group, page_group, Q * QT)

    def backward(collected, bundle):
        page_block, mask_block, sums_block, scale_block = bundle
        outputs = []
        for number in range(page_group):
            masked = masked_logits(question_embedding_matrix, page_block[number], mask_block[number])
            weights = jnp.exp(masked - sums_block[number][:, None])
            factor = (scale_block[number][:, None] * weights).astype(jnp.bfloat16)
            factor = lax.optimization_barrier(factor).astype(jnp.float32)
            collected = collected + jnp.dot(factor, page_block[number], preferred_element_type=jnp.float32)
            outputs.append(jnp.dot(factor.T, question_embedding_matrix, preferred_element_type=jnp.float32))
        return collected, jnp.stack(outputs)

    collected, grad_blocks = lax.scan(backward, jnp.zeros((Q * QT, D), jnp.float32), (grouped_pages, grouped_masks, logsumexp_results, factor_scale))
    grad_pages = grad_blocks.reshape(PAGES, PATCH, D)
    grad_queries = collected.reshape(Q, QT, D)
    return grad_queries, grad_pages, mean_loss
```

```python
import jax
import jax.numpy as jnp
from jax import lax
from jax.experimental import pallas as pl
from jax.experimental.pallas import tpu as pltpu
from jax.sharding import Mesh
from jax.sharding import PartitionSpec as P

AXES = ("xl", "y", "c", "xh", "z")
MESH = pl.DeviceIdType.MESH
F32, BF16, I32 = jnp.float32, jnp.bfloat16, jnp.int32
NZ = 16
NS = 16
TOK = 16
D = 128
ROWS = NZ * TOK
STEP = 4
FLOOR = -1e30
MARK = 128.0


def iota(shape, dim):
    return lax.broadcasted_iota(I32, shape, dim)


def exact_dot(a, b):
    return jnp.dot(a, b, preferred_element_type=F32, precision=lax.Precision.HIGHEST)


def kernel(
    q_ref,
    qmask_ref,
    pos_ref,
    pg_ref,
    pmask_ref,
    gq_ref,
    gp_ref,
    loss_ref,
    q_all,
    meta_all,
    pages,
    q_t,
    e_all,
    top,
    tot,
    logn,
    score,
    coef,
    stat,
    gq_t,
    gp_send,
    own_a,
    own_b,
    mid_a,
    mid_b,
    out_a,
    out_b,
    in_a,
    in_b,
    gq_pair,
    gq_in,
    gq_own,
    gq_send,
    gq_recv,
    loss_x,
    loss_y,
    zs_sem,
    q_recv,
    m_recv,
    pair_send,
    pair_recv,
    pg_send,
    pg_recv,
    stat_send,
    stat_recv,
    gp_ssem,
    gp_rsem,
    st2_send,
    st2_recv,
    gq_ssem,
    gq_rsem,
    loss_send,
    loss_recv,
):
    xl, y, c, xh, z = (lax.axis_index(a) for a in AXES)
    x = xh * 2 + xl
    other = 1 - c

    def at_x(d):
        t = lax.rem(x + d, 4)
        return {"xl": lax.rem(t, 2), "xh": lax.div(t, 2)}

    def at_y(d):
        return {"y": lax.rem(y + d, 4)}

    def at_z(d):
        return {"z": lax.rem(z + d, NZ)}

    pair = {"c": other}
    sends = []

    def push(src, dst, ssem, rsem, device):
        copy = pltpu.make_async_remote_copy(
            src_ref=src, dst_ref=dst, send_sem=ssem, recv_sem=rsem, device_id=device, device_id_type=MESH
        )
        copy.start()
        return copy

    def arrived(ref, sem):
        pltpu.make_async_copy(ref, ref, sem).wait()

    barrier = pltpu.get_barrier_semaphore()
    near = [s for d in range(1, STEP + 1) for s in (d, NZ - d)]
    peers = [at_z(d) for d in near] + [pair] + [at_x(d) for d in (1, 2, 3)] + [at_y(d) for d in (1, 2, 3)]
    for device in peers:
        pl.semaphore_signal(barrier, inc=1, device_id=device, device_id_type=MESH)

    prow = iota((128, 128), 0)
    for k in range(2):
        count = jnp.sum(pmask_ref[pl.ds(k, 1), :].astype(F32), axis=1, keepdims=True)
        keep = jnp.logical_or(prow < 127, jnp.broadcast_to(count, (128, 128)) > 127.5)
        pages[0, 0, k] = jnp.where(keep, pg_ref[k].astype(F32), MARK + count).astype(BF16)
    q_all[c, z] = q_ref[0]
    lane = iota((1, 128), 1)
    base = lax.rem(z, 8) * TOK
    meta = jnp.where(lax.shift_right_logical(lane, 4) == lax.rem(z, 8), pos_ref[0] * 2, 0)
    for t in range(TOK):
        meta = meta + jnp.where(lane == base + t, qmask_ref[0, t], 0)
    meta_all[c, z] = meta

    pl.semaphore_wait(barrier, len(peers))

    def send_query(zsrc, d, i):
        sends.append(push(q_all.at[c, zsrc], q_all.at[c, zsrc], zs_sem.at[0, i], q_recv.at[zsrc], at_z(d)))
        sends.append(push(meta_all.at[c, zsrc], meta_all.at[c, zsrc], zs_sem.at[1, i], m_recv.at[zsrc], at_z(d)))

    n = 0
    for d in reversed(near):
        send_query(z, d, n)
        n += 1
    for i, d in enumerate((2, 1, 3)):
        sends.append(push(pages.at[0, 0], pages.at[4 - d, 0], pg_send.at[i], pg_recv.at[0, 4 * (4 - d)], at_x(d)))
        sends.append(push(pages.at[0, 0], pages.at[0, 4 - d], pg_send.at[3 + i], pg_recv.at[0, 4 - d], at_y(d)))
    m = 6
    for d in (1, 3, 2):
        arrived(pages.at[d, 0], pg_recv.at[0, 4 * d])
        for e in (2, 1, 3):
            dst = pages.at[d, 4 - e, 0]
            sends.append(push(pages.at[d, 0, 0], dst, pg_send.at[m], pg_recv.at[0, 4 * d + 4 - e], at_y(e)))
            m += 1
        arrived(pages.at[0, d], pg_recv.at[0, d])
        for e in (2, 1, 3):
            dst = pages.at[4 - e, d, 1]
            sends.append(push(pages.at[0, d, 1], dst, pg_send.at[m], pg_recv.at[1, 4 * (4 - e) + d], at_x(e)))
            m += 1

    def got_query(d):
        zsrc = lax.rem(z + d, NZ)
        arrived(q_all.at[c, zsrc], q_recv.at[zsrc])
        arrived(meta_all.at[c, zsrc], m_recv.at[zsrc])
        return zsrc

    behind = got_query(NZ - STEP)
    for d in range(STEP, 0, -1):
        send_query(behind, d, n)
        n += 1
    ahead = got_query(STEP)
    for d in range(STEP - 1, 0, -1):
        send_query(ahead, NZ - d, n)
        n += 1
    for d in range(1, NZ):
        if d not in (STEP, NZ - STEP):
            got_query(d)
    sends.append(push(q_all.at[c], q_all.at[c], pair_send.at[0], pair_recv.at[0], pair))
    sends.append(push(meta_all.at[c], meta_all.at[c], pair_send.at[1], pair_recv.at[1], pair))
    for dx in range(1, 4):
        for dy in range(1, 4):
            arrived(pages.at[dx, dy, 0], pg_recv.at[0, 4 * dx + dy])
            arrived(pages.at[dx, dy, 1], pg_recv.at[1, 4 * dx + dy])

    def forward(h):
        rows = q_all[h].reshape(ROWS, D)
        q_t[h] = (rows.astype(F32) * 2.0).T.astype(BF16)

        def slot(s, carry):
            rx, ry = lax.div(s, 4), lax.rem(s, 4)
            for k in range(2):
                page = pages[rx, ry, k]
                last = pages[rx, ry, k, pl.ds(112, 16), :].astype(F32)[15:16]
                count = jnp.where(last > 100.0, last - MARK, 128.0)
                count = jnp.concatenate([count, count], axis=1)
                logits = jnp.dot(page, q_t[h], preferred_element_type=F32)
                live = iota((128, ROWS), 0) < count.astype(I32)
                logits = jnp.where(live, logits, FLOOR)
                highest = jnp.max(logits, axis=0, keepdims=True)
                e = jnp.exp(logits - highest)
                e_all[h, s, k] = e
                row = pl.ds(2 * s + k, 1)
                top[h, row, :] = highest
                tot[h, row, :] = jnp.sum(e, axis=0, keepdims=True)
                logn[h, row, :] = count
            return carry

        lax.fori_loop(0, NS, slot, 0)

    forward(c)
    arrived(q_all.at[other], pair_recv.at[0])
    arrived(meta_all.at[other], pair_recv.at[1])
    forward(other)

    same = lax.shift_right_logical(iota((ROWS, ROWS), 0), 4) == lax.shift_right_logical(iota((ROWS, ROWS), 1), 4)
    same = jnp.where(same, 1.0, 0.0).astype(F32)
    i = iota((32, ROWS), 0)
    px = jnp.bitwise_and(x + lax.shift_right_logical(i, 3), 3)
    py = jnp.bitwise_and(y + jnp.bitwise_and(lax.shift_right_logical(i, 1), 3), 3)
    blk = (jnp.bitwise_and(px, 1) * 4 + py) * 2 + c
    page_id = (blk * 32 + lax.shift_right_logical(px, 1) * 16 + z) * 2 + jnp.bitwise_and(i, 1)
    masks, chosen, lse_rows, picked_rows = [], [], [], []
    for h in range(2):
        lo = sum(meta_all[h, t] for t in range(8))
        hi = sum(meta_all[h, t] for t in range(8, 16))
        both = jnp.concatenate([lo, hi], axis=1)
        masks.append(jnp.bitwise_and(both, 1).astype(F32))
        chosen.append(page_id == lax.shift_right_logical(both, 1))
        lse = top[h] + jnp.log(tot[h])
        value = masks[h] * (0.5 * (lse - jnp.log(logn[h])))
        total = exact_dot(value, same)
        score[h] = total
        highest = jnp.max(total, axis=0, keepdims=True)
        lse_rows.append(highest + jnp.log(jnp.sum(jnp.exp(total - highest), axis=0, keepdims=True)))
        picked_rows.append(jnp.sum(jnp.where(chosen[h], total, 0.0), axis=0, keepdims=True))

    tok = jnp.bitwise_and(lane, 15)
    row = jnp.zeros((1, 128), F32)
    for j in range(4):
        part = slice(128 * (j % 2), 128 * (j % 2) + 128)
        piece = jnp.where(tok < 12, lse_rows[j // 2][:, part], picked_rows[j // 2][:, part])
        row = row + jnp.where(jnp.bitwise_and(tok, 3) == j, piece, 0.0)
    mine = c * NZ + z
    stat[mine] = row
    stat_sends = [push(stat.at[mine], stat.at[mine], stat_send.at[0], stat_recv.at[mine], pair)]
    for d in (8, 7, 9, 6, 10, 5, 11, 4, 12, 3, 13, 2, 14, 1, 15):
        for e, cc in ((0, c), (1, other)):
            device = {"c": cc, **at_z(d)}
            stat_sends.append(push(stat.at[mine], stat.at[mine], stat_send.at[2 * d + e], stat_recv.at[mine], device))
    sends += stat_sends
    for d in range(1, NZ):
        for cc in (c, other):
            slot_ = cc * NZ + lax.rem(z + d, NZ)
            arrived(stat.at[slot_], stat_recv.at[slot_])
    slot_ = other * NZ + z
    arrived(stat.at[slot_], stat_recv.at[slot_])
    highest = stat[0]
    for d in range(1, 32):
        highest = jnp.maximum(highest, stat[d])
    total = jnp.zeros((1, 128), F32)
    picked = jnp.zeros((1, 128), F32)
    for d in range(32):
        total = total + jnp.exp(stat[d] - highest)
        picked = picked + stat[d]
    page_lse = highest + jnp.log(total)
    part = jnp.where(tok < 4, page_lse, jnp.where(tok >= 12, -picked, 0.0))
    column_loss = jnp.broadcast_to(jnp.sum(part, axis=1, keepdims=True), (1, 128))
    loss_x[x] = column_loss
    for d in (1, 2, 3):
        sends.append(push(loss_x.at[x], loss_x.at[x], loss_send.at[d], loss_recv.at[x], at_x(d)))
    lane_in, lane_out = iota((128, 512), 0), iota((128, 512), 1)
    source = lax.shift_left(lax.shift_right_logical(jnp.bitwise_and(lane_out, 127), 4), 4) + lax.shift_right_logical(
        lane_out, 7
    )
    spread = jnp.where(lane_in == source, 1.0, 0.0).astype(F32)
    wide = exact_dot(jnp.broadcast_to(page_lse, (8, 128)), spread)[0:1]
    for h in range(2):
        coefficient = jnp.exp(score[h] - wide[:, 256 * h : 256 * h + 256]) - jnp.where(chosen[h], 1.0, 0.0)
        coef[h] = coefficient * masks[h] / tot[h]

    gq_t[...] = jnp.zeros_like(gq_t)

    def gp_copy(s, k, device, dst, rsem):
        return pltpu.make_async_remote_copy(
            src_ref=gp_send.at[s, k],
            dst_ref=dst,
            send_sem=gp_ssem.at[k, s],
            recv_sem=rsem,
            device_id=device,
            device_id_type=MESH,
        )

    def copy_a(s, rx, ry):
        back = lax.rem(4 - ry, 4)
        return gp_copy(s, 0, at_y(ry), mid_a.at[back, rx], gp_rsem.at[0, 4 * back + rx])

    def copy_b(s, rx, ry):
        back = lax.rem(4 - rx, 4)
        return gp_copy(s, 1, at_x(rx), mid_b.at[back, ry], gp_rsem.at[1, 4 * back + ry])

    def backward(t, carry):
        rx = 3 - lax.rem(t, 4)
        ry = 3 - lax.rem(lax.div(t, 4) + lax.rem(t, 4), 4)
        s = 4 * rx + ry
        factors = []
        for h in range(2):
            factors.append(
                [(e_all[h, s, k] * coef[h, pl.ds(2 * s + k, 1), :]).astype(BF16) for k in range(2)]
            )
        grads = []
        for k in range(2):
            g = jnp.dot(factors[0][k], q_all[0].reshape(ROWS, D), preferred_element_type=F32)
            g = g + jnp.dot(factors[1][k], q_all[1].reshape(ROWS, D), preferred_element_type=F32)
            grads.append(g)
            gp_send[s, k] = g.astype(BF16)

        @pl.when(ry != 0)
        def _():
            copy_a(s, rx, ry).start()

        @pl.when(ry == 0)
        def _():
            own_a[rx] = grads[0]

        @pl.when(rx != 0)
        def _():
            copy_b(s, rx, ry).start()

        @pl.when(rx == 0)
        def _():
            own_b[ry] = grads[1]

        page_t = pages[rx, ry].reshape(256, 128).T
        for h in range(2):
            gq_t[h] += jnp.dot(page_t, jnp.concatenate(factors[h], axis=0), preferred_element_type=F32)
        return carry

    lax.fori_loop(0, NS, backward, 0)

    gq_pair[...] = gq_t[other].T
    sends.append(push(gq_pair, gq_in, pair_send.at[2], pair_recv.at[2], pair))
    gq_own[...] = gq_t[c].T

    for d in (1, 2, 3):
        t = lax.rem(x + d, 4)
        arrived(loss_x.at[t], loss_recv.at[t])
    line = loss_x[0] + loss_x[1] + loss_x[2] + loss_x[3]
    loss_y[y] = line
    for d in (1, 2, 3):
        sends.append(push(loss_y.at[y], loss_y.at[y], loss_send.at[4 + d], loss_recv.at[4 + y], at_y(d)))

    arrived(gq_in, pair_recv.at[2])
    gq_own[...] += gq_in[...]
    gq_send[...] = gq_own[...].astype(BF16).reshape(NZ, TOK, D)
    for d in (8, 7, 9, 6, 10, 5, 11, 4, 12, 3, 13, 2, 14, 1, 15):
        zz = lax.rem(z + d, NZ)
        sends.append(push(gq_send.at[zz], gq_recv.at[z], gq_ssem.at[d], gq_rsem.at[z], at_z(d)))

    for r in (2, 1, 3, 0):
        acc_a, acc_b = own_a[r], own_b[r]
        for d in (1, 2, 3):
            arrived(mid_a.at[d, r], gp_rsem.at[0, 4 * d + r])
            acc_a = acc_a + mid_a[d, r].astype(F32)
            arrived(mid_b.at[d, r], gp_rsem.at[1, 4 * d + r])
            acc_b = acc_b + mid_b[d, r].astype(F32)
        if r:
            out_a[r] = acc_a.astype(BF16)
            sends.append(push(out_a.at[r], in_a.at[4 - r], st2_send.at[0, r], st2_recv.at[0, 4 - r], at_x(r)))
            out_b[r] = acc_b.astype(BF16)
            sends.append(push(out_b.at[r], in_b.at[4 - r], st2_send.at[1, r], st2_recv.at[1, 4 - r], at_y(r)))
        else:
            own_a[0] = acc_a
            own_b[0] = acc_b

    for d in (1, 2, 3):
        t = lax.rem(y + d, 4)
        arrived(loss_y.at[t], loss_recv.at[4 + t])
    loss_ref[...] = (loss_y[0] + loss_y[1] + loss_y[2] + loss_y[3]) * (1.0 / 512.0)

    for d in (1, 2, 3):
        arrived(in_a.at[d], st2_recv.at[0, d])
        arrived(in_b.at[d], st2_recv.at[1, d])
    gp_ref[0] = own_a[0] + (in_a[1].astype(F32) + in_a[2].astype(F32) + in_a[3].astype(F32))
    gp_ref[1] = own_b[0] + (in_b[1].astype(F32) + in_b[2].astype(F32) + in_b[3].astype(F32))

    total = gq_own[pl.ds(pl.multiple_of(z * TOK, TOK), TOK), :]
    for d in range(1, NZ):
        zz = lax.rem(z + d, NZ)
        arrived(gq_recv.at[zz], gq_rsem.at[zz])
        total = total + gq_recv[zz].astype(F32)
    gq_ref[0] = total

    for copy in sends:
        copy.wait_send()
    for rx in range(4):
        for ry in range(4):
            s = 4 * rx + ry
            if ry:
                copy_a(s, rx, ry).wait_send()
            if rx:
                copy_b(s, rx, ry).wait_send()


def on_device(queries, query_mask, positive, page_vectors, page_mask):
    vmem = pl.BlockSpec(memory_space=pltpu.VMEM)
    smem = pl.BlockSpec(memory_space=pltpu.SMEM)
    V = pltpu.VMEM
    dma = pltpu.SemaphoreType.DMA
    scratch = [
        V((2, NZ, TOK, D), BF16),
        V((2, NZ, 1, 128), I32),
        V((4, 4, 2, 128, D), BF16),
        V((2, D, ROWS), BF16),
        V((2, NS, 2, 128, ROWS), F32),
        V((2, 32, ROWS), F32),
        V((2, 32, ROWS), F32),
        V((2, 32, ROWS), F32),
        V((2, 32, ROWS), F32),
        V((2, 32, ROWS), F32),
        V((32, 1, 128), F32),
        V((2, D, ROWS), F32),
        V((NS, 2, 128, D), BF16),
        V((4, 128, D), F32),
        V((4, 128, D), F32),
        V((4, 4, 128, D), BF16),
        V((4, 4, 128, D), BF16),
        V((4, 128, D), BF16),
        V((4, 128, D), BF16),
        V((4, 128, D), BF16),
        V((4, 128, D), BF16),
        V((ROWS, D), F32),
        V((ROWS, D), F32),
        V((ROWS, D), F32),
        V((NZ, TOK, D), BF16),
        V((NZ, TOK, D), BF16),
        V((4, 1, 128), F32),
        V((4, 1, 128), F32),
        dma((2, 15)),
        dma((NZ,)),
        dma((NZ,)),
        dma((3,)),
        dma((3,)),
        dma((24,)),
        dma((2, 16)),
        dma((32,)),
        dma((32,)),
        dma((2, 16)),
        dma((2, 16)),
        dma((2, 4)),
        dma((2, 4)),
        dma((NZ,)),
        dma((NZ,)),
        dma((8,)),
        dma((8,)),
    ]
    gq, gp, loss = pl.pallas_call(
        kernel,
        out_shape=(
            jax.ShapeDtypeStruct((1, TOK, D), F32),
            jax.ShapeDtypeStruct((2, 128, D), F32),
            jax.ShapeDtypeStruct((1, 128), F32),
        ),
        in_specs=[vmem, smem, smem, vmem, vmem],
        out_specs=(vmem, vmem, vmem),
        scratch_shapes=scratch,
        compiler_params=pltpu.CompilerParams(collective_id=0, has_side_effects=True),
    )(queries, query_mask, positive, page_vectors, page_mask)
    return gq, gp, loss[0, 0]


def solution(mesh):
    split = Mesh(mesh.devices.reshape(2, 4, 2, 2, 16), AXES)
    return jax.shard_map(
        on_device,
        mesh=split,
        in_specs=(P(AXES, None, None), P(AXES, None), P(AXES), P(AXES, None, None), P(AXES, None)),
        out_specs=(P(AXES, None, None), P(AXES, None, None), P()),
        check_vma=False,
    )
```

```python
import jax
import jax.numpy as jnp
from jax import lax
from jax.experimental import pallas as pl
from jax.experimental.pallas import tpu as pltpu
from jax.sharding import Mesh
from jax.sharding import PartitionSpec as P

AXES = ("xl", "y", "c", "xh", "z")
MESH = pl.DeviceIdType.MESH
F32, BF16, I32 = jnp.float32, jnp.bfloat16, jnp.int32
NZ = 16
NS = 16
TOK = 16
D = 128
ROWS = NZ * TOK
STEP = 4
FLOOR = -1e30
MARK = 128.0


def iota(shape, dim):
    return lax.broadcasted_iota(I32, shape, dim)


def exact_dot(a, b):
    return jnp.dot(a, b, preferred_element_type=F32, precision=lax.Precision.HIGHEST)


def kernel(
    q_hbm,
    qmask_hbm,
    pos_hbm,
    pg_hbm,
    pmask_hbm,
    gq_ref,
    gp_ref,
    loss_ref,
    qmask,
    pos,
    pg_in,
    pmask,
    load_sem,
    q_all,
    meta_all,
    pages,
    pages_t,
    q_t,
    factor,
    e_all,
    top,
    tot,
    logn,
    score,
    coef,
    stat,
    gq_t,
    gp_send,
    own_a,
    own_b,
    mid_a,
    mid_b,
    out_a,
    out_b,
    in_a,
    in_b,
    gq_pair,
    gq_in,
    gq_own,
    gq_send,
    gq_recv,
    loss_x,
    loss_y,
    zs_sem,
    q_recv,
    m_recv,
    pair_send,
    pair_recv,
    pg_send,
    pg_recv,
    stat_send,
    stat_recv,
    gp_ssem,
    gp_rsem,
    st2_send,
    st2_recv,
    gq_ssem,
    gq_rsem,
    loss_send,
    loss_recv,
):
    xl, y, c, xh, z = (lax.axis_index(a) for a in AXES)
    x = xh * 2 + xl
    other = 1 - c

    def at_x(d):
        t = lax.rem(x + d, 4)
        return {"xl": lax.rem(t, 2), "xh": lax.div(t, 2)}

    def at_y(d):
        return {"y": lax.rem(y + d, 4)}

    def at_z(d):
        return {"z": lax.rem(z + d, NZ)}

    pair = {"c": other}
    sends = []

    scopes = []

    def phase(name):
        if scopes:
            scopes.pop().__exit__(None, None, None)
        if name:
            scopes.append(jax.named_scope(name))
            scopes[-1].__enter__()

    def push(src, dst, ssem, rsem, device):
        copy = pltpu.make_async_remote_copy(
            src_ref=src, dst_ref=dst, send_sem=ssem, recv_sem=rsem, device_id=device, device_id_type=MESH
        )
        copy.start()
        return copy

    def arrived(ref, sem):
        pltpu.make_async_copy(ref, ref, sem).wait()

    phase("entry")
    barrier = pltpu.get_barrier_semaphore()
    near = [s for d in range(1, STEP + 1) for s in (d, NZ - d)]
    peers = [at_z(d) for d in near] + [pair] + [at_x(d) for d in (1, 2, 3)] + [at_y(d) for d in (1, 2, 3)]
    for device in peers:
        pl.semaphore_signal(barrier, inc=1, device_id=device, device_id_type=MESH)

    phase("own")
    loads = [
        pltpu.make_async_copy(pg_hbm, pg_in, load_sem.at[0]),
        pltpu.make_async_copy(pmask_hbm, pmask, load_sem.at[1]),
        pltpu.make_async_copy(q_hbm.at[0], q_all.at[c, z], load_sem.at[2]),
        pltpu.make_async_copy(qmask_hbm, qmask, load_sem.at[3]),
        pltpu.make_async_copy(pos_hbm, pos, load_sem.at[4]),
    ]
    for load in loads:
        load.start()
    for load in loads:
        load.wait()
    prow = iota((128, 128), 0)
    for k in range(2):
        count = jnp.sum(pmask[pl.ds(k, 1), :].astype(F32), axis=1, keepdims=True)
        keep = jnp.logical_or(prow < 127, jnp.broadcast_to(count, (128, 128)) > 127.5)
        pages[0, 0, k] = jnp.where(keep, pg_in[k].astype(F32), MARK + count).astype(BF16)
    lane = iota((1, 128), 1)
    base = lax.rem(z, 8) * TOK
    meta = jnp.where(lax.shift_right_logical(lane, 4) == lax.rem(z, 8), pos[0] * 2, 0)
    for t in range(TOK):
        meta = meta + jnp.where(lane == base + t, qmask[0, t], 0)
    meta_all[c, z] = meta

    phase("barrier")
    pl.semaphore_wait(barrier, len(peers))

    phase("issue")

    def send_query(zsrc, d, i):
        sends.append(push(q_all.at[c, zsrc], q_all.at[c, zsrc], zs_sem.at[0, i], q_recv.at[zsrc], at_z(d)))
        sends.append(push(meta_all.at[c, zsrc], meta_all.at[c, zsrc], zs_sem.at[1, i], m_recv.at[zsrc], at_z(d)))

    n = 0
    for i, d in enumerate((2, 1, 3)):
        sends.append(push(pages.at[0, 0], pages.at[4 - d, 0], pg_send.at[i], pg_recv.at[0, 4 * (4 - d)], at_x(d)))
        sends.append(push(pages.at[0, 0], pages.at[0, 4 - d], pg_send.at[3 + i], pg_recv.at[0, 4 - d], at_y(d)))
    for d in reversed(near):
        send_query(z, d, n)
        n += 1

    def got_query(d):
        zsrc = lax.rem(z + d, NZ)
        arrived(q_all.at[c, zsrc], q_recv.at[zsrc])
        arrived(meta_all.at[c, zsrc], m_recv.at[zsrc])
        return zsrc

    phase("query_near")
    behind = got_query(NZ - STEP)
    for d in range(STEP, 0, -1):
        send_query(behind, d, n)
        n += 1
    ahead = got_query(STEP)
    for d in range(STEP - 1, 0, -1):
        send_query(ahead, NZ - d, n)
        n += 1

    phase("relay")
    m = 6
    for d in (1, 3, 2):
        arrived(pages.at[d, 0], pg_recv.at[0, 4 * d])
        for e in (2, 1, 3):
            dst = pages.at[d, 4 - e, 0]
            sends.append(push(pages.at[d, 0, 0], dst, pg_send.at[m], pg_recv.at[0, 4 * d + 4 - e], at_y(e)))
            m += 1
        arrived(pages.at[0, d], pg_recv.at[0, d])
        for e in (2, 1, 3):
            dst = pages.at[4 - e, d, 1]
            sends.append(push(pages.at[0, d, 1], dst, pg_send.at[m], pg_recv.at[1, 4 * (4 - e) + d], at_x(e)))
            m += 1

    phase("query_far")
    for d in range(1, NZ):
        if d not in (STEP, NZ - STEP):
            got_query(d)
    sends.append(push(q_all.at[c], q_all.at[c], pair_send.at[0], pair_recv.at[0], pair))
    sends.append(push(meta_all.at[c], meta_all.at[c], pair_send.at[1], pair_recv.at[1], pair))

    def turn_queries(h):
        q_t[h] = (q_all[h].reshape(ROWS, D).astype(F32) * 2.0).T.astype(BF16)

    def forward(halves, slots):
        for rx, ry in slots:
            s = 4 * rx + ry
            block = pages[rx, ry].reshape(256, D)
            lives = []
            for k in range(2):
                last = pages[rx, ry, k, pl.ds(112, 16), :].astype(F32)[15:16]
                count = jnp.where(last > 100.0, last - MARK, 128.0)
                logn[pl.ds(2 * s + k, 1), :] = count
                lives.append(prow < jnp.broadcast_to(count.astype(I32), (128, 128)))
            for h in halves:
                logits = jnp.dot(block, q_t[h], preferred_element_type=F32)
                for k in range(2):
                    for v in range(2):
                        lanes = pl.ds(128 * v, 128)
                        part = logits[128 * k : 128 * k + 128, 128 * v : 128 * v + 128]
                        part = jnp.where(lives[k], part, FLOOR)
                        highest = jnp.max(part, axis=0, keepdims=True)
                        e = jnp.exp(part - highest)
                        e_all[h, s, k, :, lanes] = e
                        top[h, pl.ds(2 * s + k, 1), lanes] = highest
                        tot[h, pl.ds(2 * s + k, 1), lanes] = jnp.sum(e, axis=0, keepdims=True)

    line_slots = [(0, 0), (1, 0), (0, 1), (3, 0), (0, 3), (2, 0), (0, 2)]
    phase("forward_own")
    turn_queries(c)
    forward([c], line_slots)
    phase("query_pair")
    arrived(q_all.at[other], pair_recv.at[0])
    arrived(meta_all.at[other], pair_recv.at[1])
    phase("forward_other")
    turn_queries(other)
    forward([other], line_slots)
    for dx in (1, 3, 2):
        phase(f"pages_{dx}")
        for dy in range(1, 4):
            arrived(pages.at[dx, dy, 0], pg_recv.at[0, 4 * dx + dy])
            arrived(pages.at[dx, dy, 1], pg_recv.at[1, 4 * dx + dy])
        phase(f"forward_{dx}")
        forward([0, 1], [(dx, dy) for dy in (1, 3, 2)])

    phase("scores")
    same = lax.shift_right_logical(iota((ROWS, ROWS), 0), 4) == lax.shift_right_logical(iota((ROWS, ROWS), 1), 4)
    same = jnp.where(same, 1.0, 0.0).astype(F32)
    i = iota((32, ROWS), 0)
    px = jnp.bitwise_and(x + lax.shift_right_logical(i, 3), 3)
    py = jnp.bitwise_and(y + jnp.bitwise_and(lax.shift_right_logical(i, 1), 3), 3)
    blk = (jnp.bitwise_and(px, 1) * 4 + py) * 2 + c
    page_id = (blk * 32 + lax.shift_right_logical(px, 1) * 16 + z) * 2 + jnp.bitwise_and(i, 1)
    log_count = jnp.log(logn[...])
    log_count = jnp.concatenate([log_count, log_count], axis=1)
    masks, chosen, lse_rows, picked_rows = [], [], [], []
    for h in range(2):
        lo = sum(meta_all[h, t] for t in range(8))
        hi = sum(meta_all[h, t] for t in range(8, 16))
        both = jnp.concatenate([lo, hi], axis=1)
        masks.append(jnp.bitwise_and(both, 1).astype(F32))
        chosen.append(page_id == lax.shift_right_logical(both, 1))
        lse = top[h] + jnp.log(tot[h])
        value = masks[h] * (0.5 * (lse - log_count))
        total = exact_dot(value, same)
        score[h] = total
        highest = jnp.max(total, axis=0, keepdims=True)
        lse_rows.append(highest + jnp.log(jnp.sum(jnp.exp(total - highest), axis=0, keepdims=True)))
        picked_rows.append(jnp.sum(jnp.where(chosen[h], total, 0.0), axis=0, keepdims=True))

    tok = jnp.bitwise_and(lane, 15)
    row = jnp.zeros((1, 128), F32)
    for j in range(4):
        part = slice(128 * (j % 2), 128 * (j % 2) + 128)
        piece = jnp.where(tok < 12, lse_rows[j // 2][:, part], picked_rows[j // 2][:, part])
        row = row + jnp.where(jnp.bitwise_and(tok, 3) == j, piece, 0.0)
    mine = c * NZ + z
    stat[mine] = row
    stat_sends = [push(stat.at[mine], stat.at[mine], stat_send.at[0], stat_recv.at[mine], pair)]
    for d in (8, 7, 9, 6, 10, 5, 11, 4, 12, 3, 13, 2, 14, 1, 15):
        for e, cc in ((0, c), (1, other)):
            device = {"c": cc, **at_z(d)}
            stat_sends.append(push(stat.at[mine], stat.at[mine], stat_send.at[2 * d + e], stat_recv.at[mine], device))
    sends += stat_sends
    phase("turn_pages")
    for s in range(NS):
        pages_t[:, pl.ds(256 * s, 256)] = pages[s // 4, s % 4].reshape(256, D).T
    phase("stat_wait")
    for d in range(1, NZ):
        for cc in (c, other):
            slot_ = cc * NZ + lax.rem(z + d, NZ)
            arrived(stat.at[slot_], stat_recv.at[slot_])
    slot_ = other * NZ + z
    arrived(stat.at[slot_], stat_recv.at[slot_])
    phase("softmax")
    highest = stat[0]
    for d in range(1, 32):
        highest = jnp.maximum(highest, stat[d])
    total = jnp.zeros((1, 128), F32)
    picked = jnp.zeros((1, 128), F32)
    for d in range(32):
        total = total + jnp.exp(stat[d] - highest)
        picked = picked + stat[d]
    page_lse = highest + jnp.log(total)
    part = jnp.where(tok < 4, page_lse, jnp.where(tok >= 12, -picked, 0.0))
    column_loss = jnp.broadcast_to(jnp.sum(part, axis=1, keepdims=True), (1, 128))
    loss_x[x] = column_loss
    for d in (1, 2, 3):
        sends.append(push(loss_x.at[x], loss_x.at[x], loss_send.at[d], loss_recv.at[x], at_x(d)))
    lane_in, lane_out = iota((128, 512), 0), iota((128, 512), 1)
    source = lax.shift_left(lax.shift_right_logical(jnp.bitwise_and(lane_out, 127), 4), 4) + lax.shift_right_logical(
        lane_out, 7
    )
    spread = jnp.where(lane_in == source, 1.0, 0.0).astype(F32)
    wide = exact_dot(jnp.broadcast_to(page_lse, (8, 128)), spread)[0:1]
    for h in range(2):
        coefficient = jnp.exp(score[h] - wide[:, 256 * h : 256 * h + 256]) - jnp.where(chosen[h], 1.0, 0.0)
        coef[h] = coefficient * masks[h] / tot[h]

    phase("backward")
    queries = q_all[...].reshape(2 * ROWS, D)
    for rx in (2, 1, 3, 0):
        for ry in (2, 1, 3, 0):
            s = 4 * rx + ry
            rows = pl.ds(256 * s, 256)
            for h in range(2):
                for k in range(2):
                    value = e_all[h, s, k] * coef[h, pl.ds(2 * s + k, 1), :]
                    factor[pl.ds(256 * s + 128 * k, 128), pl.ds(ROWS * h, ROWS)] = value.astype(BF16)
            grads = jnp.dot(factor[rows, :], queries, preferred_element_type=F32)
            grads_a, grads_b = grads[:128], grads[128:]
            if ry:
                gp_send[s, 0] = grads_a.astype(BF16)
                rsem = gp_rsem.at[0, 4 * (4 - ry) + rx]
                sends.append(push(gp_send.at[s, 0], mid_a.at[4 - ry, rx], gp_ssem.at[0, s], rsem, at_y(ry)))
            else:
                own_a[rx] = grads_a
            if rx:
                gp_send[s, 1] = grads_b.astype(BF16)
                rsem = gp_rsem.at[1, 4 * (4 - rx) + ry]
                sends.append(push(gp_send.at[s, 1], mid_b.at[4 - rx, ry], gp_ssem.at[1, s], rsem, at_x(rx)))
            else:
                own_b[ry] = grads_b
    phase("grad_queries")
    for h in range(2):
        gq_t[h] = jnp.dot(pages_t[...], factor[:, pl.ds(ROWS * h, ROWS)], preferred_element_type=F32)

    phase("turn")
    gq_pair[...] = gq_t[other].T
    sends.append(push(gq_pair, gq_in, pair_send.at[2], pair_recv.at[2], pair))
    gq_own[...] = gq_t[c].T

    phase("loss_line")
    for d in (1, 2, 3):
        t = lax.rem(x + d, 4)
        arrived(loss_x.at[t], loss_recv.at[t])
    line = loss_x[0] + loss_x[1] + loss_x[2] + loss_x[3]
    loss_y[y] = line
    for d in (1, 2, 3):
        sends.append(push(loss_y.at[y], loss_y.at[y], loss_send.at[4 + d], loss_recv.at[4 + y], at_y(d)))

    phase("gq_pair")
    arrived(gq_in, pair_recv.at[2])
    gq_own[...] += gq_in[...]
    gq_send[...] = gq_own[...].astype(BF16).reshape(NZ, TOK, D)
    for d in (8, 7, 9, 6, 10, 5, 11, 4, 12, 3, 13, 2, 14, 1, 15):
        zz = lax.rem(z + d, NZ)
        sends.append(push(gq_send.at[zz], gq_recv.at[z], gq_ssem.at[d], gq_rsem.at[z], at_z(d)))

    phase("lines")
    for r in (2, 1, 3, 0):
        acc_a, acc_b = own_a[r], own_b[r]
        for d in (1, 2, 3):
            arrived(mid_a.at[d, r], gp_rsem.at[0, 4 * d + r])
            acc_a = acc_a + mid_a[d, r].astype(F32)
            arrived(mid_b.at[d, r], gp_rsem.at[1, 4 * d + r])
            acc_b = acc_b + mid_b[d, r].astype(F32)
        if r:
            out_a[r] = acc_a.astype(BF16)
            sends.append(push(out_a.at[r], in_a.at[4 - r], st2_send.at[0, r], st2_recv.at[0, 4 - r], at_x(r)))
            out_b[r] = acc_b.astype(BF16)
            sends.append(push(out_b.at[r], in_b.at[4 - r], st2_send.at[1, r], st2_recv.at[1, 4 - r], at_y(r)))
        else:
            own_a[0] = acc_a
            own_b[0] = acc_b

    phase("loss")
    for d in (1, 2, 3):
        t = lax.rem(y + d, 4)
        arrived(loss_y.at[t], loss_recv.at[4 + t])
    loss_ref[...] = (loss_y[0] + loss_y[1] + loss_y[2] + loss_y[3]) * (1.0 / 512.0)

    phase("gp_last")
    for d in (1, 2, 3):
        arrived(in_a.at[d], st2_recv.at[0, d])
        arrived(in_b.at[d], st2_recv.at[1, d])
    gp_ref[0] = own_a[0] + (in_a[1].astype(F32) + in_a[2].astype(F32) + in_a[3].astype(F32))
    gp_ref[1] = own_b[0] + (in_b[1].astype(F32) + in_b[2].astype(F32) + in_b[3].astype(F32))

    phase("gq_last")
    total = gq_own[pl.ds(pl.multiple_of(z * TOK, TOK), TOK), :]
    for d in range(1, NZ):
        zz = lax.rem(z + d, NZ)
        arrived(gq_recv.at[zz], gq_rsem.at[zz])
        total = total + gq_recv[zz].astype(F32)
    gq_ref[0] = total

    phase("drain")
    for copy in sends:
        copy.wait_send()
    phase(None)


def write_out(gq_in, gp_in, loss_in, gq_hbm, gp_hbm, loss_out, sem):
    copies = [
        pltpu.make_async_copy(gp_in, gp_hbm, sem.at[0]),
        pltpu.make_async_copy(gq_in, gq_hbm, sem.at[1]),
    ]
    for copy in copies:
        copy.start()
    loss_out[0] = loss_in[0, 0]
    for copy in copies:
        copy.wait()


def on_device(queries, query_mask, positive, page_vectors, page_mask):
    hbm = pl.BlockSpec(memory_space=pl.ANY)
    vmem = pl.BlockSpec(memory_space=pltpu.VMEM)
    smem = pl.BlockSpec(memory_space=pltpu.SMEM)
    V = pltpu.VMEM
    dma = pltpu.SemaphoreType.DMA
    scratch = [
        pltpu.SMEM((1, TOK), I32),
        pltpu.SMEM((1,), I32),
        V((2, 128, D), BF16),
        V((2, 128), I32),
        dma((5,)),
        V((2, NZ, TOK, D), BF16),
        V((2, NZ, 1, 128), I32),
        V((4, 4, 2, 128, D), BF16),
        V((D, NS * 256), BF16),
        V((2, D, ROWS), BF16),
        V((NS * 256, 2 * ROWS), BF16),
        V((2, NS, 2, 128, ROWS), F32),
        V((2, 32, ROWS), F32),
        V((2, 32, ROWS), F32),
        V((32, 128), F32),
        V((2, 32, ROWS), F32),
        V((2, 32, ROWS), F32),
        V((32, 1, 128), F32),
        V((2, D, ROWS), F32),
        V((NS, 2, 128, D), BF16),
        V((4, 128, D), F32),
        V((4, 128, D), F32),
        V((4, 4, 128, D), BF16),
        V((4, 4, 128, D), BF16),
        V((4, 128, D), BF16),
        V((4, 128, D), BF16),
        V((4, 128, D), BF16),
        V((4, 128, D), BF16),
        V((ROWS, D), F32),
        V((ROWS, D), F32),
        V((ROWS, D), F32),
        V((NZ, TOK, D), BF16),
        V((NZ, TOK, D), BF16),
        V((4, 1, 128), F32),
        V((4, 1, 128), F32),
        dma((2, 15)),
        dma((NZ,)),
        dma((NZ,)),
        dma((3,)),
        dma((3,)),
        dma((24,)),
        dma((2, 16)),
        dma((32,)),
        dma((32,)),
        dma((2, 16)),
        dma((2, 16)),
        dma((2, 4)),
        dma((2, 4)),
        dma((NZ,)),
        dma((NZ,)),
        dma((8,)),
        dma((8,)),
    ]
    partial = pl.pallas_call(
        kernel,
        out_shape=(V((1, TOK, D), F32), V((2, 128, D), F32), V((1, 128), F32)),
        in_specs=[hbm] * 5,
        out_specs=(vmem, vmem, vmem),
        scratch_shapes=scratch,
        compiler_params=pltpu.CompilerParams(collective_id=0, has_side_effects=True),
    )(queries, query_mask, positive, page_vectors, page_mask)
    gq, gp, loss = pl.pallas_call(
        write_out,
        out_shape=(
            jax.ShapeDtypeStruct((1, TOK, D), F32),
            jax.ShapeDtypeStruct((2, 128, D), F32),
            jax.ShapeDtypeStruct((1,), F32),
        ),
        in_specs=[vmem] * 3,
        out_specs=(hbm, hbm, smem),
        scratch_shapes=[dma((2,))],
        compiler_params=pltpu.CompilerParams(vmem_limit_bytes=1 << 20),
    )(*[pltpu.with_memory_space_constraint(p, pltpu.VMEM) for p in partial])
    return gq, gp, loss.reshape(())


def solution(mesh):
    split = Mesh(mesh.devices.reshape(2, 4, 2, 2, 16), AXES)
    return jax.shard_map(
        on_device,
        mesh=split,
        in_specs=(P(AXES, None, None), P(AXES, None), P(AXES), P(AXES, None, None), P(AXES, None)),
        out_specs=(P(AXES, None, None), P(AXES, None, None), P()),
        check_vma=False,
    )
```

```python
import jax
import jax.numpy as jnp
from jax import lax
from jax.experimental import pallas as pl
from jax.experimental.pallas import tpu as pltpu
from jax.sharding import Mesh
from jax.sharding import PartitionSpec as P

AXES = ("xl", "y", "c", "xh", "z")
MESH = pl.DeviceIdType.MESH
F32, BF16, I32 = jnp.float32, jnp.bfloat16, jnp.int32
NZ = 16
NS = 16
TOK = 16
D = 128
ROWS = NZ * TOK
STEP = 4
FLOOR = -1e30
MARK = 128.0


def iota(shape, dim):
    return lax.broadcasted_iota(I32, shape, dim)


def exact_dot(a, b):
    return jnp.dot(a, b, preferred_element_type=F32, precision=lax.Precision.HIGHEST)


def kernel(
    q_hbm,
    qmask_hbm,
    pos_hbm,
    pg_hbm,
    pmask_hbm,
    gq_ref,
    gp_ref,
    loss_ref,
    qmask,
    pos,
    pg_in,
    pmask,
    load_sem,
    q_all,
    pages,
    pages_t,
    q_t,
    factor,
    e_all,
    top,
    tot,
    logn,
    score,
    coef,
    stat,
    gq_t,
    gp_send,
    own_a,
    own_b,
    mid_a,
    mid_b,
    out_a,
    out_b,
    in_a,
    in_b,
    gq_pair,
    gq_in,
    gq_own,
    gq_send,
    gq_recv,
    loss_x,
    loss_y,
    q_send,
    q_recv,
    pair_send,
    pair_recv,
    pg_send,
    line_recv,
    far_recv,
    stat_sem,
    gp_send_sem,
    gp_recv,
    st2_send,
    st2_recv,
    gq_sem,
    loss_sem,
):
    xl, y, c, xh, z = (lax.axis_index(a) for a in AXES)
    x = xh * 2 + xl
    other = 1 - c

    def at_x(d):
        t = lax.rem(x + d, 4)
        return {"xl": lax.rem(t, 2), "xh": lax.div(t, 2)}

    def at_y(d):
        return {"y": lax.rem(y + d, 4)}

    def at_z(d):
        return {"z": lax.rem(z + d, NZ)}

    pair = {"c": other}

    scopes = []

    def phase(name):
        if scopes:
            scopes.pop().__exit__(None, None, None)
        if name:
            scopes.append(jax.named_scope(name))
            scopes[-1].__enter__()

    def push(src, dst, ssem, rsem, device):
        copy = pltpu.make_async_remote_copy(
            src_ref=src, dst_ref=dst, send_sem=ssem, recv_sem=rsem, device_id=device, device_id_type=MESH
        )
        copy.start()

    def arrived(ref, sem):
        pltpu.make_async_copy(ref, ref, sem).wait()

    phase("entry")
    barrier = pltpu.get_barrier_semaphore()
    near = [s for d in range(1, STEP + 1) for s in (d, NZ - d)]
    peers = [at_z(d) for d in near] + [pair] + [at_x(d) for d in (1, 2, 3)] + [at_y(d) for d in (1, 2, 3)]
    for device in peers:
        pl.semaphore_signal(barrier, inc=1, device_id=device, device_id_type=MESH)

    phase("own")
    loads = [
        pltpu.make_async_copy(pg_hbm, pg_in, load_sem.at[0]),
        pltpu.make_async_copy(pmask_hbm, pmask, load_sem.at[1]),
        pltpu.make_async_copy(q_hbm.at[0], q_all.at[c, z, pl.ds(0, TOK)], load_sem.at[2]),
        pltpu.make_async_copy(qmask_hbm, qmask, load_sem.at[3]),
        pltpu.make_async_copy(pos_hbm, pos, load_sem.at[4]),
    ]
    for load in loads:
        load.start()
    for load in loads:
        load.wait()
    prow = iota((128, 128), 0)
    for k in range(2):
        count = jnp.sum(pmask[pl.ds(k, 1), :].astype(F32), axis=1, keepdims=True)
        keep = jnp.logical_or(prow < 127, jnp.broadcast_to(count, (128, 128)) > 127.5)
        pages[0, k] = jnp.where(keep, pg_in[k].astype(F32), MARK + count).astype(BF16)
    lane = iota((1, 128), 1)
    base = lax.rem(z, 8) * TOK
    mask = jnp.zeros((1, 128), I32)
    for t in range(TOK):
        mask = mask + jnp.where(lane == base + t, qmask[0, t], 0)
    group = lax.shift_right_logical(lane, 4) == lax.rem(z, 8)
    page_hi = jnp.where(group, lax.shift_right_logical(pos[0, 0], 5), 0)
    page_lo = jnp.where(group, jnp.bitwise_and(pos[0, 0], 31), 0)
    mrow = iota((8, 128), 0)
    meta = jnp.where(mrow == 0, mask, jnp.where(mrow == 1, page_hi, jnp.where(mrow == 2, page_lo, 0)))
    q_all[c, z, pl.ds(TOK, 8), :] = meta.astype(F32).astype(BF16)

    phase("barrier")
    pl.semaphore_wait(barrier, len(peers))

    phase("issue")

    def send_query(zsrc, d, i):
        push(q_all.at[c, zsrc], q_all.at[c, zsrc], q_send, q_recv.at[i], at_z(d))

    for d in (2, 1, 3):
        push(pages.at[0, 0], pages.at[4 * (4 - d), 0], pg_send, line_recv.at[0, d - 1], at_x(d))
        push(pages.at[0, 1], pages.at[4 - d, 1], pg_send, line_recv.at[1, d - 1], at_y(d))
    for d in (2, 1, 3):
        push(pages.at[0, 1], pages.at[4 * (4 - d), 1], pg_send, far_recv.at[0], at_x(d))
        push(pages.at[0, 0], pages.at[4 - d, 0], pg_send, far_recv.at[0], at_y(d))

    for d in reversed(near):
        send_query(z, d, 0 if d == STEP else 1 if d == NZ - STEP else 2)

    def got_query(d, i):
        zsrc = lax.rem(z + d, NZ)
        arrived(q_all.at[c, zsrc], q_recv.at[i])
        return zsrc

    phase("relay")
    for d in (1, 3, 2):
        arrived(pages.at[4 * d, 0], line_recv.at[0, 3 - d])
        for e in (2, 1, 3):
            push(pages.at[4 * d, 0], pages.at[4 * d + 4 - e, 0], pg_send, far_recv.at[d], at_y(e))
        arrived(pages.at[d, 1], line_recv.at[1, 3 - d])
        for e in (2, 1, 3):
            push(pages.at[d, 1], pages.at[4 * (4 - e) + d, 1], pg_send, far_recv.at[4 - e], at_x(e))

    phase("query_near")
    behind = got_query(NZ - STEP, 0)
    for d in range(STEP, 0, -1):
        send_query(behind, d, 2)
    ahead = got_query(STEP, 1)
    for d in range(STEP - 1, 0, -1):
        send_query(ahead, NZ - d, 2)

    phase("query_far")
    arrived(q_all.at[c, pl.ds(0, 13)], q_recv.at[2])
    push(q_all.at[c], q_all.at[c], pair_send.at[0], pair_recv.at[0], pair)

    def turn_queries(h):
        q_t[h] = (q_all[h, :, pl.ds(0, TOK), :].reshape(ROWS, D).astype(F32) * 2.0).T.astype(BF16)

    def forward(h, slots):
        for rx, ry in slots:
            s = 4 * rx + ry
            for k in range(2):
                last = pages[s, k, pl.ds(112, 16), :].astype(F32)[15:16]
                count = jnp.where(last > 100.0, last - MARK, 128.0)
                live = prow < jnp.broadcast_to(count.astype(I32), (128, 128))
                row = pl.ds(2 * s + k, 1)
                logn[row, :] = count
                logits = jnp.dot(pages[s, k], q_t[h], preferred_element_type=F32)
                for v in range(2):
                    lanes = pl.ds(128 * v, 128)
                    part = jnp.where(live, logits[:, 128 * v : 128 * v + 128], FLOOR)
                    highest = jnp.max(part, axis=0, keepdims=True)
                    e = jnp.exp(part - highest)
                    e_all[h, s, k, :, lanes] = e
                    top[h, row, lanes] = highest
                    tot[h, row, lanes] = jnp.sum(e, axis=0, keepdims=True)

    line_slots = [(0, 0), (1, 0), (0, 1), (3, 0), (0, 3), (2, 0), (0, 2)]
    far_slots = [(dx, dy) for dx in (1, 3, 2) for dy in (1, 3, 2)]
    phase("forward_own")
    turn_queries(c)
    arrived(pages.at[pl.ds(0, 3)], far_recv.at[0])
    forward(c, line_slots)
    phase("pages_far")
    for dx in (1, 2, 3):
        arrived(pages.at[pl.ds(4 * dx + 1, 3)], far_recv.at[dx])
    phase("forward_far")
    forward(c, far_slots)
    phase("query_pair")
    arrived(q_all.at[other], pair_recv.at[0])
    phase("forward_other")
    turn_queries(other)
    forward(other, line_slots + far_slots)

    phase("scores")
    same = lax.shift_right_logical(iota((ROWS, ROWS), 0), 4) == lax.shift_right_logical(iota((ROWS, ROWS), 1), 4)
    same = jnp.where(same, 1.0, 0.0).astype(F32)
    i = iota((32, ROWS), 0)
    px = jnp.bitwise_and(x + lax.shift_right_logical(i, 3), 3)
    py = jnp.bitwise_and(y + jnp.bitwise_and(lax.shift_right_logical(i, 1), 3), 3)
    blk = (jnp.bitwise_and(px, 1) * 4 + py) * 2 + c
    page_id = (blk * 32 + lax.shift_right_logical(px, 1) * 16 + z) * 2 + jnp.bitwise_and(i, 1)
    log_count = jnp.log(logn[...])
    log_count = jnp.concatenate([log_count, log_count], axis=1)
    masks, chosen, lse_rows, picked_rows = [], [], [], []
    for h in range(2):
        lo = sum(q_all[h, t, pl.ds(TOK, 8), :].astype(F32) for t in range(8))
        hi = sum(q_all[h, t, pl.ds(TOK, 8), :].astype(F32) for t in range(8, 16))
        both = jnp.concatenate([lo, hi], axis=1)
        masks.append(both[0:1])
        chosen.append(page_id.astype(F32) == both[1:2] * 32.0 + both[2:3])
        lse = top[h] + jnp.log(tot[h])
        value = masks[h] * (0.5 * (lse - log_count))
        total = exact_dot(value, same)
        score[h] = total
        highest = jnp.max(total, axis=0, keepdims=True)
        lse_rows.append(highest + jnp.log(jnp.sum(jnp.exp(total - highest), axis=0, keepdims=True)))
        picked_rows.append(jnp.sum(jnp.where(chosen[h], total, 0.0), axis=0, keepdims=True))

    tok = jnp.bitwise_and(lane, 15)
    row = jnp.zeros((1, 128), F32)
    for j in range(4):
        part = slice(128 * (j % 2), 128 * (j % 2) + 128)
        piece = jnp.where(tok < 12, lse_rows[j // 2][:, part], picked_rows[j // 2][:, part])
        row = row + jnp.where(jnp.bitwise_and(tok, 3) == j, piece, 0.0)
    mine = c * NZ + z
    stat[mine] = row
    push(stat.at[mine], stat.at[mine], stat_sem.at[0], stat_sem.at[1], pair)
    for d in (8, 7, 9, 6, 10, 5, 11, 4, 12, 3, 13, 2, 14, 1, 15):
        for cc in (c, other):
            push(stat.at[mine], stat.at[mine], stat_sem.at[0], stat_sem.at[1], {"c": cc, **at_z(d)})
    order = []
    for r in (2, 1, 3, 0):
        for d in (2, 1, 3):
            order += [(4 * r + d, 0), (4 * d + r, 1)]
    order += [(4 * r, 0) for r in range(4)] + [(r, 1) for r in range(4)]
    phase("turn_pages")
    for i, (s, k) in enumerate(order):
        pages_t[:, pl.ds(128 * i, 128)] = pages[s, k].T
    phase("stat_wait")
    arrived(stat.at[pl.ds(0, 31)], stat_sem.at[1])
    phase("softmax")
    highest = stat[0]
    for d in range(1, 32):
        highest = jnp.maximum(highest, stat[d])
    total = jnp.zeros((1, 128), F32)
    picked = jnp.zeros((1, 128), F32)
    for d in range(32):
        total = total + jnp.exp(stat[d] - highest)
        picked = picked + stat[d]
    page_lse = highest + jnp.log(total)
    part = jnp.where(tok < 4, page_lse, jnp.where(tok >= 12, -picked, 0.0))
    column_loss = jnp.broadcast_to(jnp.sum(part, axis=1, keepdims=True), (1, 128))
    loss_x[x] = column_loss
    for d in (1, 2, 3):
        push(loss_x.at[x], loss_x.at[x], loss_sem.at[0], loss_sem.at[1], at_x(d))
    lane_in, lane_out = iota((128, 512), 0), iota((128, 512), 1)
    source = lax.shift_left(lax.shift_right_logical(jnp.bitwise_and(lane_out, 127), 4), 4) + lax.shift_right_logical(
        lane_out, 7
    )
    spread = jnp.where(lane_in == source, 1.0, 0.0).astype(F32)
    wide = exact_dot(jnp.broadcast_to(page_lse, (8, 128)), spread)[0:1]
    for h in range(2):
        coefficient = jnp.exp(score[h] - wide[:, 256 * h : 256 * h + 256]) - jnp.where(chosen[h], 1.0, 0.0)
        coef[h] = coefficient * masks[h] / tot[h]

    phase("backward")
    queries = q_all[:, :, pl.ds(0, TOK), :].reshape(2 * ROWS, D)

    def form_factor(i):
        s, k = order[i]
        for h in range(2):
            value = e_all[h, s, k] * coef[h, pl.ds(2 * s + k, 1), :]
            factor[pl.ds(128 * i, 128), pl.ds(ROWS * h, ROWS)] = value.astype(BF16)

    def page_grads(start, size):
        grads = jnp.dot(factor[pl.ds(128 * start, 128 * size), :], queries, preferred_element_type=F32)
        for i in range(size):
            s, k = order[start + i]
            rx, ry = s // 4, s % 4
            g = grads[128 * i : 128 * i + 128]
            if k == 0 and ry:
                gp_send[s, 0] = g.astype(BF16)
                push(gp_send.at[s, 0], mid_a.at[rx, 3 - ry], gp_send_sem, gp_recv.at[0, rx], at_y(ry))
            elif k == 0:
                own_a[rx] = g
            elif rx:
                gp_send[s, 1] = g.astype(BF16)
                push(gp_send.at[s, 1], mid_b.at[ry, 3 - rx], gp_send_sem, gp_recv.at[1, ry], at_x(rx))
            else:
                own_b[ry] = g

    def query_grads():
        for h in range(2):
            gq_t[h] = jnp.dot(pages_t[...], factor[:, pl.ds(ROWS * h, ROWS)], preferred_element_type=F32)
        gq_pair[...] = gq_t[other].T
        push(gq_pair, gq_in, pair_send.at[1], pair_recv.at[1], pair)
        gq_own[...] = gq_t[c].T

    def query_grads_away():
        arrived(gq_in, pair_recv.at[1])
        gq_own[...] += gq_in[...]
        gq_send[...] = gq_own[...].astype(BF16).reshape(NZ, TOK, D)
        for d in (8, 7, 9, 6, 10, 5, 11, 4, 12, 3, 13, 2, 14, 1, 15):
            zz = lax.rem(z + d, NZ)
            push(gq_send.at[zz], gq_recv.at[z], gq_sem.at[0], gq_sem.at[1], at_z(d))

    @pl.when(z < 4)
    def _():
        for start in range(0, 32, 4):
            for i in range(4):
                form_factor(start + i)
            page_grads(start, 4)
        query_grads()
        query_grads_away()

    @pl.when(z >= 4)
    def _():
        for i in range(32):
            form_factor(i)
        query_grads()
        for start in range(0, 16, 4):
            page_grads(start, 4)
        query_grads_away()
        for start in range(16, 32, 4):
            page_grads(start, 4)

    phase("loss_line")
    arrived(loss_x.at[pl.ds(0, 3)], loss_sem.at[1])
    line = loss_x[0] + loss_x[1] + loss_x[2] + loss_x[3]
    loss_y[y] = line
    for d in (1, 2, 3):
        push(loss_y.at[y], loss_y.at[y], loss_sem.at[2], loss_sem.at[3], at_y(d))

    phase("lines")
    for r in (2, 1, 3, 0):
        arrived(mid_a.at[r], gp_recv.at[0, r])
        acc_a = own_a[r] + (mid_a[r, 0].astype(F32) + mid_a[r, 1].astype(F32) + mid_a[r, 2].astype(F32))
        arrived(mid_b.at[r], gp_recv.at[1, r])
        acc_b = own_b[r] + (mid_b[r, 0].astype(F32) + mid_b[r, 1].astype(F32) + mid_b[r, 2].astype(F32))
        if r:
            out_a[r - 1] = acc_a.astype(BF16)
            push(out_a.at[r - 1], in_a.at[3 - r], st2_send.at[0], st2_recv.at[0], at_x(r))
            out_b[r - 1] = acc_b.astype(BF16)
            push(out_b.at[r - 1], in_b.at[3 - r], st2_send.at[1], st2_recv.at[1], at_y(r))
        else:
            own_a[0] = acc_a
            own_b[0] = acc_b

    phase("loss")
    arrived(loss_y.at[pl.ds(0, 3)], loss_sem.at[3])
    loss_ref[...] = (loss_y[0] + loss_y[1] + loss_y[2] + loss_y[3]) * (1.0 / 512.0)

    phase("gp_last")
    arrived(in_a, st2_recv.at[0])
    gp_ref[0] = own_a[0] + (in_a[0].astype(F32) + in_a[1].astype(F32) + in_a[2].astype(F32))
    arrived(in_b, st2_recv.at[1])
    gp_ref[1] = own_b[0] + (in_b[0].astype(F32) + in_b[1].astype(F32) + in_b[2].astype(F32))

    phase("gq_last")
    total = gq_own[pl.ds(pl.multiple_of(z * TOK, TOK), TOK), :]
    arrived(gq_recv.at[pl.ds(0, NZ - 1)], gq_sem.at[1])
    for d in range(1, NZ):
        zz = lax.rem(z + d, NZ)
        total = total + gq_recv[zz].astype(F32)
    gq_ref[0] = total

    phase("drain")
    arrived(q_all.at[c, pl.ds(0, NZ - 1)], q_send)
    arrived(pages.at[pl.ds(0, NS - 1)], pg_send)
    arrived(q_all.at[c], pair_send.at[0])
    arrived(gq_pair, pair_send.at[1])
    arrived(stat.at[pl.ds(0, 31)], stat_sem.at[0])
    arrived(gp_send.at[pl.ds(0, 12)], gp_send_sem)
    arrived(out_a, st2_send.at[0])
    arrived(out_b, st2_send.at[1])
    arrived(gq_send.at[pl.ds(0, NZ - 1)], gq_sem.at[0])
    arrived(loss_x.at[pl.ds(0, 3)], loss_sem.at[0])
    arrived(loss_y.at[pl.ds(0, 3)], loss_sem.at[2])
    phase(None)


def write_out(gq_in, gp_in, loss_in, gq_hbm, gp_hbm, loss_out, sem):
    copies = [
        pltpu.make_async_copy(gp_in, gp_hbm, sem.at[0]),
        pltpu.make_async_copy(gq_in, gq_hbm, sem.at[1]),
    ]
    for copy in copies:
        copy.start()
    loss_out[0] = loss_in[0, 0]
    for copy in copies:
        copy.wait()


def on_device(queries, query_mask, positive, page_vectors, page_mask):
    hbm = pl.BlockSpec(memory_space=pl.ANY)
    vmem = pl.BlockSpec(memory_space=pltpu.VMEM)
    smem = pl.BlockSpec(memory_space=pltpu.SMEM)
    V = pltpu.VMEM
    dma = pltpu.SemaphoreType.DMA
    scratch = [
        pltpu.SMEM((1, TOK), I32),
        pltpu.SMEM((1, 1), I32),
        V((2, 128, D), BF16),
        V((2, 128), I32),
        dma((5,)),
        V((2, NZ, TOK + 8, D), BF16),
        V((NS, 2, 128, D), BF16),
        V((D, NS * 256), BF16),
        V((2, D, ROWS), BF16),
        V((NS * 256, 2 * ROWS), BF16),
        V((2, NS, 2, 128, ROWS), F32),
        V((2, 32, ROWS), F32),
        V((2, 32, ROWS), F32),
        V((32, 128), F32),
        V((2, 32, ROWS), F32),
        V((2, 32, ROWS), F32),
        V((32, 1, 128), F32),
        V((2, D, ROWS), F32),
        V((NS, 2, 128, D), BF16),
        V((4, 128, D), F32),
        V((4, 128, D), F32),
        V((4, 3, 128, D), BF16),
        V((4, 3, 128, D), BF16),
        V((3, 128, D), BF16),
        V((3, 128, D), BF16),
        V((3, 128, D), BF16),
        V((3, 128, D), BF16),
        V((ROWS, D), F32),
        V((ROWS, D), F32),
        V((ROWS, D), F32),
        V((NZ, TOK, D), BF16),
        V((NZ, TOK, D), BF16),
        V((4, 1, 128), F32),
        V((4, 1, 128), F32),
        dma(()),
        dma((3,)),
        dma((2,)),
        dma((2,)),
        dma(()),
        dma((2, 3)),
        dma((4,)),
        dma((2,)),
        dma(()),
        dma((2, 4)),
        dma((2,)),
        dma((2,)),
        dma((2,)),
        dma((4,)),
    ]
    partial = pl.pallas_call(
        kernel,
        out_shape=(V((1, TOK, D), F32), V((2, 128, D), F32), V((1, 128), F32)),
        in_specs=[hbm] * 5,
        out_specs=(vmem, vmem, vmem),
        scratch_shapes=scratch,
        compiler_params=pltpu.CompilerParams(collective_id=0, has_side_effects=True),
    )(queries, query_mask, positive.reshape(1, 1), page_vectors, page_mask)
    gq, gp, loss = pl.pallas_call(
        write_out,
        out_shape=(
            jax.ShapeDtypeStruct((1, TOK, D), F32),
            jax.ShapeDtypeStruct((2, 128, D), F32),
            jax.ShapeDtypeStruct((1,), F32),
        ),
        in_specs=[vmem] * 3,
        out_specs=(hbm, hbm, smem),
        scratch_shapes=[dma((2,))],
        compiler_params=pltpu.CompilerParams(vmem_limit_bytes=1 << 20),
    )(*[pltpu.with_memory_space_constraint(p, pltpu.VMEM) for p in partial])
    return gq, gp, loss.reshape(())


def solution(mesh):
    split = Mesh(mesh.devices.reshape(2, 4, 2, 2, 16), AXES)
    return jax.shard_map(
        on_device,
        mesh=split,
        in_specs=(P(AXES, None, None), P(AXES, None), P(AXES), P(AXES, None, None), P(AXES, None)),
        out_specs=(P(AXES, None, None), P(AXES, None, None), P()),
        check_vma=False,
    )
```

```python
import math

import jax
import jax.numpy as jnp
from jax import lax
from jax.experimental import pallas as pl
from jax.experimental.pallas import tpu as pltpu
from jax.sharding import Mesh
from jax.sharding import PartitionSpec as P

AXES = ("xl", "y", "c", "xh", "z")
MESH = pl.DeviceIdType.MESH
F32, BF16, I32 = jnp.float32, jnp.bfloat16, jnp.int32
NZ = 16
NS = 16
TOK = 16
D = 128
ROWS = NZ * TOK
STEP = 4
FLOOR = -1e30
RATE = 2.0 * math.log2(math.e)
MARK = 128.0


def iota(shape, dim):
    return lax.broadcasted_iota(I32, shape, dim)


def select_dot(a, chooser):
    parts, rest = [], a
    for _ in range(3):
        parts.append(rest.astype(BF16))
        rest = rest - parts[-1].astype(F32)
    n = a.shape[0]
    out = jnp.dot(jnp.concatenate(parts, axis=0), chooser, preferred_element_type=F32)
    return out[:n] + out[n : 2 * n] + out[2 * n :]


def kernel(
    q_hbm,
    qmask_hbm,
    pos_hbm,
    pg_hbm,
    pmask_hbm,
    gq_ref,
    gp_ref,
    loss_ref,
    qmask,
    pos,
    pg_in,
    pmask,
    load_sem,
    q_all,
    pages,
    pages_t,
    q_t,
    bias,
    same,
    spread,
    factor,
    e_all,
    top,
    tot,
    logn,
    score,
    coef,
    stat,
    gq_t,
    gp_send,
    own_a,
    own_b,
    mid_a,
    mid_b,
    out_a,
    out_b,
    in_a,
    in_b,
    gq_pair,
    gq_in,
    gq_own,
    gq_send,
    gq_recv,
    loss_x,
    loss_y,
    q_send,
    q_recv,
    pair_send,
    pair_recv,
    pg_send,
    line_recv,
    far_recv,
    stat_sem,
    gp_send_sem,
    gp_recv,
    st2_send,
    st2_recv,
    gq_sem,
    loss_sem,
):
    xl, y, c, xh, z = (lax.axis_index(a) for a in AXES)
    x = xh * 2 + xl
    other = 1 - c

    def at_x(d):
        t = lax.rem(x + d, 4)
        return {"xl": lax.rem(t, 2), "xh": lax.div(t, 2)}

    def at_y(d):
        return {"y": lax.rem(y + d, 4)}

    def at_z(d):
        return {"z": lax.rem(z + d, NZ)}

    pair = {"c": other}

    scopes = []

    def phase(name):
        if scopes:
            scopes.pop().__exit__(None, None, None)
        if name:
            scopes.append(jax.named_scope(name))
            scopes[-1].__enter__()

    def push(src, dst, ssem, rsem, device):
        copy = pltpu.make_async_remote_copy(
            src_ref=src, dst_ref=dst, send_sem=ssem, recv_sem=rsem, device_id=device, device_id_type=MESH
        )
        copy.start()

    def arrived(ref, sem):
        pltpu.make_async_copy(ref, ref, sem).wait()

    phase("entry")
    barrier = pltpu.get_barrier_semaphore()
    near = [s for d in range(1, STEP + 1) for s in (d, NZ - d)]
    peers = [at_z(d) for d in near] + [pair] + [at_x(d) for d in (1, 2, 3)] + [at_y(d) for d in (1, 2, 3)]
    for device in peers:
        pl.semaphore_signal(barrier, inc=1, device_id=device, device_id_type=MESH)

    phase("own")
    loads = [
        pltpu.make_async_copy(pg_hbm, pg_in, load_sem.at[0]),
        pltpu.make_async_copy(pmask_hbm, pmask, load_sem.at[1]),
        pltpu.make_async_copy(q_hbm.at[0], q_all.at[c, z, pl.ds(0, TOK)], load_sem.at[2]),
        pltpu.make_async_copy(qmask_hbm, qmask, load_sem.at[3]),
        pltpu.make_async_copy(pos_hbm, pos, load_sem.at[4]),
    ]
    for load in loads:
        load.start()
    krow = iota((D, ROWS), 0)
    for h in range(2):
        q_t[h, pl.ds(D, D), :] = jnp.where(krow == 0, 1.0, 0.0).astype(BF16)
    together = lax.shift_right_logical(iota((ROWS, ROWS), 0), 4) == lax.shift_right_logical(iota((ROWS, ROWS), 1), 4)
    same[...] = jnp.where(together, 1.0, 0.0).astype(BF16)
    lane_out = iota((128, 512), 1)
    source = jnp.bitwise_and(lane_out, 112) + lax.shift_right_logical(lane_out, 7)
    spread[...] = jnp.where(iota((128, 512), 0) == source, 1.0, 0.0).astype(BF16)
    for load in loads:
        load.wait()
    prow = iota((128, 128), 0)
    for k in range(2):
        count = jnp.sum(pmask[pl.ds(k, 1), :].astype(F32), axis=1, keepdims=True)
        keep = jnp.logical_or(prow < 127, jnp.broadcast_to(count, (128, 128)) > 127.5)
        pages[0, k] = jnp.where(keep, pg_in[k].astype(F32), MARK + count).astype(BF16)
    lane = iota((1, 128), 1)
    base = lax.rem(z, 8) * TOK
    mask = jnp.zeros((1, 128), I32)
    for t in range(TOK):
        mask = mask + jnp.where(lane == base + t, qmask[0, t], 0)
    group = lax.shift_right_logical(lane, 4) == lax.rem(z, 8)
    page_hi = jnp.where(group, lax.shift_right_logical(pos[0], 5), 0)
    page_lo = jnp.where(group, jnp.bitwise_and(pos[0], 31), 0)
    mrow = iota((8, 128), 0)
    meta = jnp.where(mrow == 0, mask, jnp.where(mrow == 1, page_hi, jnp.where(mrow == 2, page_lo, 0)))
    q_all[c, z, pl.ds(TOK, 8), :] = meta.astype(F32).astype(BF16)

    phase("barrier")
    pl.semaphore_wait(barrier, len(peers))

    phase("issue")

    for d in reversed(near):
        sem = q_recv.at[0 if d == STEP else 1 if d == NZ - STEP else 2]
        push(q_all.at[c, z], q_all.at[c, z], q_send.at[0], sem, at_z(d))

    def pass_query(zsrc, d):
        push(q_all.at[c, zsrc], q_all.at[c, zsrc], q_send.at[0], q_recv.at[3], at_z(d))
        push(q_all.at[c, zsrc], q_all.at[c, zsrc], q_send.at[1], q_recv.at[5], {"c": other, **at_z(d)})

    for d in (2, 1, 3):
        push(pages.at[0, 0], pages.at[4 * (4 - d), 0], pg_send, line_recv.at[0, d - 1], at_x(d))
        push(pages.at[0, 1], pages.at[4 - d, 1], pg_send, line_recv.at[1, d - 1], at_y(d))
    for d in (2, 1, 3):
        push(pages.at[0, 1], pages.at[4 * (4 - d), 1], pg_send, far_recv.at[0], at_x(d))
        push(pages.at[0, 0], pages.at[4 - d, 0], pg_send, far_recv.at[0], at_y(d))

    def relay(d):
        arrived(pages.at[4 * d, 0], line_recv.at[0, 3 - d])
        for e in (2, 1, 3):
            push(pages.at[4 * d, 0], pages.at[4 * d + 4 - e, 0], pg_send, far_recv.at[1], at_y(e))
        arrived(pages.at[d, 1], line_recv.at[1, 3 - d])
        for e in (2, 1, 3):
            push(pages.at[d, 1], pages.at[4 * (4 - e) + d, 1], pg_send, far_recv.at[1], at_x(e))

    phase("relay")
    relay(1)
    relay(3)
    phase("query_near")
    arrived(q_all.at[c, pl.ds(0, 6)], q_recv.at[2])
    behind, ahead = lax.rem(z + NZ - STEP, NZ), lax.rem(z + STEP, NZ)
    arrived(q_all.at[c, behind], q_recv.at[0])
    arrived(q_all.at[c, ahead], q_recv.at[1])
    for d in range(STEP, 0, -1):
        pass_query(behind, d)
    for d in range(STEP - 1, 0, -1):
        pass_query(ahead, NZ - d)
    for d in [0] + near:
        zsrc = lax.rem(z + d, NZ)
        push(q_all.at[c, zsrc], q_all.at[c, zsrc], q_send.at[1], q_recv.at[4], pair)
    phase("relay_2")
    relay(2)

    def turn_queries(h):
        q_t[h, pl.ds(0, D), :] = q_all[h, :, pl.ds(0, TOK), :].reshape(ROWS, D).T

    first = iota((128, 128), 1) == 0

    def count_patches(slots):
        for rx, ry in slots:
            s = 4 * rx + ry
            for k in range(2):
                last = pages[s, k, pl.ds(112, 16), :].astype(F32)[15:16]
                count = jnp.where(last > 100.0, last - MARK, 128.0)
                logn[pl.ds(2 * s + k, 1), :] = count
                unused = jnp.logical_and(first, prow >= jnp.broadcast_to(count.astype(I32), (128, 128)))
                bias[s, pl.ds(128 * k, 128), :] = jnp.where(unused, FLOOR, 0.0).astype(BF16)

    def forward(h, slots):
        for rx, ry in slots:
            s = 4 * rx + ry
            block = jnp.concatenate([pages[s].reshape(256, D), bias[s]], axis=1)
            dots = jnp.dot(block, q_t[h], preferred_element_type=F32)
            for k in range(2):
                row = pl.ds(2 * s + k, 1)
                for v in range(2):
                    lanes = pl.ds(128 * v, 128)
                    part = dots[128 * k : 128 * k + 128, 128 * v : 128 * v + 128]
                    highest = jnp.max(part, axis=0, keepdims=True)
                    e = jnp.exp2((part - highest) * RATE)
                    e_all[h, s, k, :, lanes] = e
                    top[h, row, lanes] = highest * 2.0
                    tot[h, row, lanes] = jnp.sum(e, axis=0, keepdims=True)

    line_slots = [(0, 0), (1, 0), (0, 1), (3, 0), (0, 3), (2, 0), (0, 2)]
    far_slots = [(dx, dy) for dx in (1, 3, 2) for dy in (1, 3, 2)]
    arrived(pages.at[pl.ds(0, 3)], far_recv.at[0])
    count_patches(line_slots)
    def own_far():
        arrived(q_all.at[c, pl.ds(0, 7)], q_recv.at[3])

    def other_core():
        arrived(q_all.at[other, pl.ds(0, 9)], q_recv.at[4])
        arrived(q_all.at[other, pl.ds(0, 7)], q_recv.at[5])

    phase("query_far")
    pl.when(c == 1)(own_far)
    pl.when(c == 0)(other_core)
    phase("forward_1")
    turn_queries(1)
    forward(1, line_slots)
    phase("query_pair")
    pl.when(c == 0)(own_far)
    pl.when(c == 1)(other_core)
    phase("forward_0")
    turn_queries(0)
    forward(0, line_slots)
    phase("pages_far")
    arrived(pages.at[pl.ds(0, 9)], far_recv.at[1])
    phase("forward_far")
    count_patches(far_slots)
    forward(1, far_slots)
    forward(0, far_slots)

    phase("scores")
    i = iota((32, ROWS), 0)
    px = jnp.bitwise_and(x + lax.shift_right_logical(i, 3), 3)
    py = jnp.bitwise_and(y + jnp.bitwise_and(lax.shift_right_logical(i, 1), 3), 3)
    blk = (jnp.bitwise_and(px, 1) * 4 + py) * 2 + c
    page_id = (blk * 32 + lax.shift_right_logical(px, 1) * 16 + z) * 2 + jnp.bitwise_and(i, 1)
    log_count = jnp.log(logn[...])
    log_count = jnp.concatenate([log_count, log_count], axis=1)
    masks, chosen, lse_rows, picked_rows = [], [], [], []
    for h in range(2):
        lo = sum(q_all[h, t, pl.ds(TOK, 8), :].astype(F32) for t in range(8))
        hi = sum(q_all[h, t, pl.ds(TOK, 8), :].astype(F32) for t in range(8, 16))
        both = jnp.concatenate([lo, hi], axis=1)
        masks.append(both[0:1])
        chosen.append(page_id.astype(F32) == both[1:2] * 32.0 + both[2:3])
        lse = top[h] + jnp.log(tot[h])
        value = masks[h] * (0.5 * (lse - log_count))
        total = select_dot(value, same[...])
        score[h] = total
        highest = jnp.max(total, axis=0, keepdims=True)
        lse_rows.append(highest + jnp.log(jnp.sum(jnp.exp(total - highest), axis=0, keepdims=True)))
        picked_rows.append(jnp.sum(jnp.where(chosen[h], total, 0.0), axis=0, keepdims=True))

    tok = jnp.bitwise_and(lane, 15)
    row = jnp.zeros((1, 128), F32)
    for j in range(4):
        part = slice(128 * (j % 2), 128 * (j % 2) + 128)
        piece = jnp.where(tok < 12, lse_rows[j // 2][:, part], picked_rows[j // 2][:, part])
        row = row + jnp.where(jnp.bitwise_and(tok, 3) == j, piece, 0.0)
    mine = c * NZ + z
    stat[mine] = row
    push(stat.at[mine], stat.at[mine], stat_sem.at[0], stat_sem.at[1], pair)
    for d in (8, 7, 9, 6, 10, 5, 11, 4, 12, 3, 13, 2, 14, 1, 15):
        for cc in (c, other):
            push(stat.at[mine], stat.at[mine], stat_sem.at[0], stat_sem.at[1], {"c": cc, **at_z(d)})
    order = []
    for r in (2, 1, 3, 0):
        for d in (2, 1, 3):
            order += [(4 * r + d, 0), (4 * d + r, 1)]
    order += [(4 * r, 0) for r in range(4)] + [(r, 1) for r in range(4)]
    phase("turn_pages")
    for i, (s, k) in enumerate(order):
        pages_t[:, pl.ds(128 * i, 128)] = pages[s, k].T
    phase("stat_wait")
    arrived(stat.at[pl.ds(0, 31)], stat_sem.at[1])
    phase("softmax")
    highest = stat[0]
    for d in range(1, 32):
        highest = jnp.maximum(highest, stat[d])
    total = jnp.zeros((1, 128), F32)
    picked = jnp.zeros((1, 128), F32)
    for d in range(32):
        total = total + jnp.exp(stat[d] - highest)
        picked = picked + stat[d]
    page_lse = highest + jnp.log(total)
    part = jnp.where(tok < 4, page_lse, jnp.where(tok >= 12, -picked, 0.0))
    column_loss = jnp.broadcast_to(jnp.sum(part, axis=1, keepdims=True), (1, 128))
    loss_x[x] = column_loss
    for d in (1, 2, 3):
        push(loss_x.at[x], loss_x.at[x], loss_sem.at[0], loss_sem.at[1], at_x(d))
    wide = select_dot(jnp.broadcast_to(page_lse, (8, 128)), spread[...])[0:1]
    for h in range(2):
        coefficient = jnp.exp(score[h] - wide[:, 256 * h : 256 * h + 256]) - jnp.where(chosen[h], 1.0, 0.0)
        coef[h] = coefficient * masks[h] / tot[h]

    phase("backward")
    queries = q_all[:, :, pl.ds(0, TOK), :].reshape(2 * ROWS, D)

    def form_factor(i):
        s, k = order[i]
        for h in range(2):
            value = e_all[h, s, k] * coef[h, pl.ds(2 * s + k, 1), :]
            factor[pl.ds(128 * i, 128), pl.ds(ROWS * h, ROWS)] = value.astype(BF16)

    def page_grads(start, stop):
        size = 2 if stop - start == 4 else 4
        for part in range(start, stop, size):
            grads = jnp.dot(factor[pl.ds(128 * part, 128 * size), :], queries, preferred_element_type=F32)
            for i in range(size):
                s, k = order[part + i]
                rx, ry = s // 4, s % 4
                g = grads[128 * i : 128 * i + 128]
                if (rx if k else ry) == 0:
                    (own_b if k else own_a)[ry if k else rx] = g
                else:
                    gp_send[s, k] = g.astype(BF16)
        for s, k in order[start:stop]:
            rx, ry = s // 4, s % 4
            if k == 0 and ry:
                push(gp_send.at[s, 0], mid_a.at[rx, 3 - ry], gp_send_sem, gp_recv.at[0, rx], at_y(ry))
            elif k == 1 and rx:
                push(gp_send.at[s, 1], mid_b.at[ry, 3 - rx], gp_send_sem, gp_recv.at[1, ry], at_x(rx))

    def query_grads():
        for h in range(2):
            gq_t[h] = jnp.dot(pages_t[...], factor[:, pl.ds(ROWS * h, ROWS)], preferred_element_type=F32)
        gq_pair[...] = gq_t[other].T
        push(gq_pair, gq_in, pair_send, pair_recv, pair)
        gq_own[...] = gq_t[c].T

    def query_grads_away():
        arrived(gq_in, pair_recv)
        gq_own[...] += gq_in[...]
        gq_send[...] = gq_own[...].astype(BF16).reshape(NZ, TOK, D)
        for d in (8, 7, 9, 6, 10, 5, 11, 4, 12, 3, 13, 2, 14, 1, 15):
            zz = lax.rem(z + d, NZ)
            push(gq_send.at[zz], gq_recv.at[z], gq_sem.at[0], gq_sem.at[1], at_z(d))

    def line_sum(r):
        arrived(mid_a.at[r], gp_recv.at[0, r])
        acc_a = own_a[r] + (mid_a[r, 0].astype(F32) + mid_a[r, 1].astype(F32) + mid_a[r, 2].astype(F32))
        if r:
            out_a[r - 1] = acc_a.astype(BF16)
            push(out_a.at[r - 1], in_a.at[3 - r], st2_send.at[0], st2_recv.at[0], at_x(r))
        else:
            own_a[0] = acc_a
        arrived(mid_b.at[r], gp_recv.at[1, r])
        acc_b = own_b[r] + (mid_b[r, 0].astype(F32) + mid_b[r, 1].astype(F32) + mid_b[r, 2].astype(F32))
        if r:
            out_b[r - 1] = acc_b.astype(BF16)
            push(out_b.at[r - 1], in_b.at[3 - r], st2_send.at[1], st2_recv.at[1], at_y(r))
        else:
            own_b[0] = acc_b

    def pass_loss():
        arrived(loss_x.at[pl.ds(0, 3)], loss_sem.at[1])
        line = loss_x[0] + loss_x[1] + loss_x[2] + loss_x[3]
        loss_y[y] = line
        for d in (1, 2, 3):
            push(loss_y.at[y], loss_y.at[y], loss_sem.at[2], loss_sem.at[3], at_y(d))

    @pl.when(z < 4)
    def _():
        for start, stop in ((0, 4), (4, 8), (8, 16), (16, 24), (24, 32)):
            for i in range(start, stop):
                form_factor(i)
            page_grads(start, stop)
        query_grads()
        pass_loss()
        line_sum(2)
        query_grads_away()

    @pl.when(z >= 4)
    def _():
        for i in range(32):
            form_factor(i)
        query_grads()
        page_grads(0, 8)
        page_grads(8, 16)
        query_grads_away()
        page_grads(16, 24)
        page_grads(24, 32)
        pass_loss()
        line_sum(2)

    phase("lines")
    line_sum(1)
    line_sum(3)
    phase("line_own")
    line_sum(0)

    phase("loss")
    arrived(loss_y.at[pl.ds(0, 3)], loss_sem.at[3])
    loss_ref[...] = (loss_y[0] + loss_y[1] + loss_y[2] + loss_y[3]) * (1.0 / 512.0)

    phase("gp_last")
    arrived(in_a, st2_recv.at[0])
    gp_ref[0] = own_a[0] + (in_a[0].astype(F32) + in_a[1].astype(F32) + in_a[2].astype(F32))
    arrived(in_b, st2_recv.at[1])
    gp_ref[1] = own_b[0] + (in_b[0].astype(F32) + in_b[1].astype(F32) + in_b[2].astype(F32))

    phase("gq_last")
    total = gq_own[pl.ds(pl.multiple_of(z * TOK, TOK), TOK), :]
    arrived(gq_recv.at[pl.ds(0, NZ - 1)], gq_sem.at[1])
    for d in range(1, NZ):
        zz = lax.rem(z + d, NZ)
        total = total + gq_recv[zz].astype(F32)
    gq_ref[0] = total

    phase("drain")
    arrived(q_all.at[c, pl.ds(0, NZ - 1)], q_send.at[0])
    arrived(q_all.at[c], q_send.at[1])
    arrived(pages.at[pl.ds(0, NS - 1)], pg_send)
    arrived(gq_pair, pair_send)
    arrived(stat.at[pl.ds(0, 31)], stat_sem.at[0])
    arrived(gp_send.at[pl.ds(0, 12)], gp_send_sem)
    arrived(out_a, st2_send.at[0])
    arrived(out_b, st2_send.at[1])
    arrived(gq_send.at[pl.ds(0, NZ - 1)], gq_sem.at[0])
    arrived(loss_x.at[pl.ds(0, 3)], loss_sem.at[0])
    arrived(loss_y.at[pl.ds(0, 3)], loss_sem.at[2])
    phase(None)


def write_out(gq_in, gp_in, loss_in, gq_hbm, gp_hbm, loss_out, sem):
    copies = [
        pltpu.make_async_copy(gp_in, gp_hbm, sem.at[0]),
        pltpu.make_async_copy(gq_in, gq_hbm, sem.at[1]),
    ]
    for copy in copies:
        copy.start()
    loss_out[0] = loss_in[0, 0]
    for copy in copies:
        copy.wait()


def on_device(queries, query_mask, positive, page_vectors, page_mask):
    hbm = pl.BlockSpec(memory_space=pl.ANY)
    vmem = pl.BlockSpec(memory_space=pltpu.VMEM)
    smem = pl.BlockSpec(memory_space=pltpu.SMEM)
    V = pltpu.VMEM
    dma = pltpu.SemaphoreType.DMA
    scratch = [
        pltpu.SMEM((1, TOK), I32),
        pltpu.SMEM((1,), I32),
        V((2, 128, D), BF16),
        V((2, 128), I32),
        dma((5,)),
        V((2, NZ, TOK + 8, D), BF16),
        V((NS, 2, 128, D), BF16),
        V((D, NS * 256), BF16),
        V((2, 2 * D, ROWS), BF16),
        V((NS, 256, 128), BF16),
        V((ROWS, ROWS), BF16),
        V((128, 512), BF16),
        V((NS * 256, 2 * ROWS), BF16),
        V((2, NS, 2, 128, ROWS), F32),
        V((2, 32, ROWS), F32),
        V((2, 32, ROWS), F32),
        V((32, 128), F32),
        V((2, 32, ROWS), F32),
        V((2, 32, ROWS), F32),
        V((32, 1, 128), F32),
        V((2, D, ROWS), F32),
        V((NS, 2, 128, D), BF16),
        V((4, 128, D), F32),
        V((4, 128, D), F32),
        V((4, 3, 128, D), BF16),
        V((4, 3, 128, D), BF16),
        V((3, 128, D), BF16),
        V((3, 128, D), BF16),
        V((3, 128, D), BF16),
        V((3, 128, D), BF16),
        V((ROWS, D), F32),
        V((ROWS, D), F32),
        V((ROWS, D), F32),
        V((NZ, TOK, D), BF16),
        V((NZ, TOK, D), BF16),
        V((4, 1, 128), F32),
        V((4, 1, 128), F32),
        dma((2,)),
        dma((6,)),
        dma(()),
        dma(()),
        dma(()),
        dma((2, 3)),
        dma((2,)),
        dma((2,)),
        dma(()),
        dma((2, 4)),
        dma((2,)),
        dma((2,)),
        dma((2,)),
        dma((4,)),
    ]
    partial = pl.pallas_call(
        kernel,
        out_shape=(V((1, TOK, D), F32), V((2, 128, D), F32), V((1, 128), F32)),
        in_specs=[hbm, hbm, pl.BlockSpec(memory_space=pltpu.HBM), hbm, hbm],
        out_specs=(vmem, vmem, vmem),
        scratch_shapes=scratch,
        compiler_params=pltpu.CompilerParams(collective_id=0, has_side_effects=True),
    )(queries, query_mask, positive, page_vectors, page_mask)
    gq, gp, loss = pl.pallas_call(
        write_out,
        out_shape=(
            jax.ShapeDtypeStruct((1, TOK, D), F32),
            jax.ShapeDtypeStruct((2, 128, D), F32),
            jax.ShapeDtypeStruct((1,), F32),
        ),
        in_specs=[vmem] * 3,
        out_specs=(hbm, hbm, smem),
        scratch_shapes=[dma((2,))],
        compiler_params=pltpu.CompilerParams(vmem_limit_bytes=1 << 20),
    )(*[pltpu.with_memory_space_constraint(p, pltpu.VMEM) for p in partial])
    return gq, gp, loss.reshape(())


def solution(mesh):
    split = Mesh(mesh.devices.reshape(2, 4, 2, 2, 16), AXES)
    return jax.shard_map(
        on_device,
        mesh=split,
        in_specs=(P(AXES, None, None), P(AXES, None), P(AXES), P(AXES, None, None), P(AXES, None)),
        out_specs=(P(AXES, None, None), P(AXES, None, None), P()),
        check_vma=False,
    )
```

```python
import math

import jax
import jax.numpy as jnp
from jax import lax
from jax.experimental import pallas as pl
from jax.experimental.pallas import tpu as pltpu
from jax.sharding import Mesh
from jax.sharding import PartitionSpec as P

AXES = ("xl", "y", "c", "xh", "z")
MESH = pl.DeviceIdType.MESH
F32, BF16, I32 = jnp.float32, jnp.bfloat16, jnp.int32
NZ = 16
NS = 16
TOK = 16
D = 128
ROWS = NZ * TOK
STEP = 4
FLOOR = -1e30
RATE = 2.0 * math.log2(math.e)
MARK = 128.0


def iota(shape, dim):
    return lax.broadcasted_iota(I32, shape, dim)


def select_dot(a, chooser):
    parts, rest = [], a
    for _ in range(3):
        parts.append(rest.astype(BF16))
        rest = rest - parts[-1].astype(F32)
    n = a.shape[0]
    out = jnp.dot(jnp.concatenate(parts, axis=0), chooser, preferred_element_type=F32)
    return out[:n] + out[n : 2 * n] + out[2 * n :]


def kernel(
    q_hbm,
    qmask_hbm,
    pos_hbm,
    pg_hbm,
    pmask_hbm,
    gq_ref,
    gp_ref,
    loss_ref,
    qmask,
    pos,
    pg_in,
    pmask,
    load_sem,
    q_all,
    pages,
    pages_t,
    q_t,
    bias,
    same,
    spread,
    factor,
    e_all,
    top,
    tot,
    logn,
    score,
    coef,
    stat,
    gq_t,
    gp_send,
    own_a,
    own_b,
    mid_a,
    mid_b,
    out_a,
    out_b,
    in_a,
    in_b,
    gq_pair,
    gq_in,
    gq_own,
    gq_send,
    gq_recv,
    loss_x,
    loss_y,
    q_send,
    q_recv,
    pair_send,
    pair_recv,
    pg_send,
    line_recv,
    far_recv,
    stat_sem,
    gp_send_sem,
    gp_recv,
    st2_send,
    st2_recv,
    gq_sem,
    loss_sem,
):
    xl, y, c, xh, z = (lax.axis_index(a) for a in AXES)
    x = xh * 2 + xl
    other = 1 - c

    def at_x(d):
        t = lax.rem(x + d, 4)
        return {"xl": lax.rem(t, 2), "xh": lax.div(t, 2)}

    def at_y(d):
        return {"y": lax.rem(y + d, 4)}

    def at_z(d):
        return {"z": lax.rem(z + d, NZ)}

    pair = {"c": other}

    scopes = []

    def phase(name):
        if scopes:
            scopes.pop().__exit__(None, None, None)
        if name:
            scopes.append(jax.named_scope(name))
            scopes[-1].__enter__()

    def push(src, dst, ssem, rsem, device):
        copy = pltpu.make_async_remote_copy(
            src_ref=src, dst_ref=dst, send_sem=ssem, recv_sem=rsem, device_id=device, device_id_type=MESH
        )
        copy.start()

    def arrived(ref, sem):
        pltpu.make_async_copy(ref, ref, sem).wait()

    phase("entry")
    barrier = pltpu.get_barrier_semaphore()
    near = [s for d in range(1, STEP + 1) for s in (d, NZ - d)]
    peers = [at_z(d) for d in near] + [pair] + [at_x(d) for d in (1, 2, 3)] + [at_y(d) for d in (1, 2, 3)]
    for device in peers:
        pl.semaphore_signal(barrier, inc=1, device_id=device, device_id_type=MESH)

    phase("own")
    loads = [
        pltpu.make_async_copy(pg_hbm, pg_in, load_sem.at[0]),
        pltpu.make_async_copy(pmask_hbm, pmask, load_sem.at[1]),
        pltpu.make_async_copy(q_hbm.at[0], q_all.at[c, z, pl.ds(0, TOK)], load_sem.at[2]),
        pltpu.make_async_copy(qmask_hbm, qmask, load_sem.at[3]),
        pltpu.make_async_copy(pos_hbm, pos, load_sem.at[4]),
    ]
    for load in loads:
        load.start()
    krow = iota((D, ROWS), 0)
    for h in range(2):
        q_t[h, pl.ds(D, D), :] = jnp.where(krow == 0, 1.0, 0.0).astype(BF16)
    together = lax.shift_right_logical(iota((ROWS, ROWS), 0), 4) == lax.shift_right_logical(iota((ROWS, ROWS), 1), 4)
    same[...] = jnp.where(together, 1.0, 0.0).astype(BF16)
    lane_out = iota((128, 512), 1)
    source = jnp.bitwise_and(lane_out, 112) + lax.shift_right_logical(lane_out, 7)
    spread[...] = jnp.where(iota((128, 512), 0) == source, 1.0, 0.0).astype(BF16)
    for load in loads:
        load.wait()
    prow = iota((128, 128), 0)
    for k in range(2):
        count = jnp.sum(pmask[pl.ds(k, 1), :].astype(F32), axis=1, keepdims=True)
        keep = jnp.logical_or(prow < 127, jnp.broadcast_to(count, (128, 128)) > 127.5)
        pages[0, k] = jnp.where(keep, pg_in[k].astype(F32), MARK + count).astype(BF16)
    lane = iota((1, 128), 1)
    base = lax.rem(z, 8) * TOK
    mask = jnp.zeros((1, 128), I32)
    for t in range(TOK):
        mask = mask + jnp.where(lane == base + t, qmask[0, t], 0)
    group = lax.shift_right_logical(lane, 4) == lax.rem(z, 8)
    page_hi = jnp.where(group, lax.shift_right_logical(pos[0], 5), 0)
    page_lo = jnp.where(group, jnp.bitwise_and(pos[0], 31), 0)
    mrow = iota((8, 128), 0)
    meta = jnp.where(mrow == 0, mask, jnp.where(mrow == 1, page_hi, jnp.where(mrow == 2, page_lo, 0)))
    q_all[c, z, pl.ds(TOK, 8), :] = meta.astype(F32).astype(BF16)

    phase("barrier")
    pl.semaphore_wait(barrier, len(peers))

    phase("issue")

    for d in reversed(near):
        sem = q_recv.at[0 if d == STEP else 1 if d == NZ - STEP else 2]
        push(q_all.at[c, z], q_all.at[c, z], q_send.at[0], sem, at_z(d))

    def pass_query(zsrc, d):
        push(q_all.at[c, zsrc], q_all.at[c, zsrc], q_send.at[0], q_recv.at[3], at_z(d))
        push(q_all.at[c, zsrc], q_all.at[c, zsrc], q_send.at[1], q_recv.at[5], {"c": other, **at_z(d)})

    for d in (2, 1, 3):
        push(pages.at[0, 0], pages.at[4 * (4 - d), 0], pg_send, line_recv.at[0, d - 1], at_x(d))
        push(pages.at[0, 1], pages.at[4 - d, 1], pg_send, line_recv.at[1, d - 1], at_y(d))
    for d in (2, 1, 3):
        push(pages.at[0, 1], pages.at[4 * (4 - d), 1], pg_send, far_recv.at[0], at_x(d))
        push(pages.at[0, 0], pages.at[4 - d, 0], pg_send, far_recv.at[0], at_y(d))

    def relay(d):
        arrived(pages.at[4 * d, 0], line_recv.at[0, 3 - d])
        for e in (2, 1, 3):
            push(pages.at[4 * d, 0], pages.at[4 * d + 4 - e, 0], pg_send, far_recv.at[1], at_y(e))
        arrived(pages.at[d, 1], line_recv.at[1, 3 - d])
        for e in (2, 1, 3):
            push(pages.at[d, 1], pages.at[4 * (4 - e) + d, 1], pg_send, far_recv.at[1], at_x(e))

    phase("relay")
    relay(1)
    relay(3)
    phase("query_near")
    arrived(q_all.at[c, pl.ds(0, 6)], q_recv.at[2])
    behind, ahead = lax.rem(z + NZ - STEP, NZ), lax.rem(z + STEP, NZ)
    arrived(q_all.at[c, behind], q_recv.at[0])
    arrived(q_all.at[c, ahead], q_recv.at[1])
    for d in range(STEP, 0, -1):
        pass_query(behind, d)
    for d in range(STEP - 1, 0, -1):
        pass_query(ahead, NZ - d)
    for d in [0] + near:
        zsrc = lax.rem(z + d, NZ)
        push(q_all.at[c, zsrc], q_all.at[c, zsrc], q_send.at[1], q_recv.at[4], pair)
    phase("relay_2")
    relay(2)

    def turn_queries(h):
        q_t[h, pl.ds(0, D), :] = q_all[h, :, pl.ds(0, TOK), :].reshape(ROWS, D).T

    first = iota((128, 128), 1) == 0

    def count_patches(slots):
        for rx, ry in slots:
            s = 4 * rx + ry
            for k in range(2):
                last = pages[s, k, pl.ds(112, 16), :].astype(F32)[15:16]
                count = jnp.where(last > 100.0, last - MARK, 128.0)
                logn[pl.ds(2 * s + k, 1), :] = count
                unused = jnp.logical_and(first, prow >= jnp.broadcast_to(count.astype(I32), (128, 128)))
                bias[s, pl.ds(128 * k, 128), :] = jnp.where(unused, FLOOR, 0.0).astype(BF16)

    def forward(h, slots):
        for rx, ry in slots:
            s = 4 * rx + ry
            block = jnp.concatenate([pages[s].reshape(256, D), bias[s]], axis=1)
            dots = jnp.dot(block, q_t[h], preferred_element_type=F32)
            for k in range(2):
                row = pl.ds(2 * s + k, 1)
                for v in range(2):
                    lanes = pl.ds(128 * v, 128)
                    part = dots[128 * k : 128 * k + 128, 128 * v : 128 * v + 128]
                    highest = jnp.max(part, axis=0, keepdims=True)
                    e = jnp.exp2((part - highest) * RATE)
                    e_all[h, s, k, :, lanes] = e
                    top[h, row, lanes] = highest * 2.0
                    tot[h, row, lanes] = jnp.sum(e, axis=0, keepdims=True)

    line_slots = [(0, 0), (1, 0), (0, 1), (3, 0), (0, 3), (2, 0), (0, 2)]
    far_slots = [(dx, dy) for dx in (1, 3, 2) for dy in (1, 3, 2)]
    arrived(pages.at[pl.ds(0, 3)], far_recv.at[0])
    count_patches(line_slots)
    def own_far():
        arrived(q_all.at[c, pl.ds(0, 7)], q_recv.at[3])

    def other_core():
        arrived(q_all.at[other, pl.ds(0, 9)], q_recv.at[4])
        arrived(q_all.at[other, pl.ds(0, 7)], q_recv.at[5])

    phase("query_far")
    pl.when(c == 1)(own_far)
    pl.when(c == 0)(other_core)
    phase("forward_1")
    turn_queries(1)
    forward(1, line_slots)
    phase("pages_far")
    arrived(pages.at[pl.ds(0, 9)], far_recv.at[1])
    phase("forward_far")
    count_patches(far_slots)
    forward(1, far_slots)
    phase("query_pair")
    pl.when(c == 0)(own_far)
    pl.when(c == 1)(other_core)
    phase("forward_0")
    turn_queries(0)
    forward(0, line_slots + far_slots)

    phase("scores")
    i = iota((32, ROWS), 0)
    px = jnp.bitwise_and(x + lax.shift_right_logical(i, 3), 3)
    py = jnp.bitwise_and(y + jnp.bitwise_and(lax.shift_right_logical(i, 1), 3), 3)
    blk = (jnp.bitwise_and(px, 1) * 4 + py) * 2 + c
    page_id = (blk * 32 + lax.shift_right_logical(px, 1) * 16 + z) * 2 + jnp.bitwise_and(i, 1)
    log_count = jnp.log(logn[...])
    log_count = jnp.concatenate([log_count, log_count], axis=1)
    masks, chosen, lse_rows, picked_rows = [], [], [], []
    for h in range(2):
        lo = sum(q_all[h, t, pl.ds(TOK, 8), :].astype(F32) for t in range(8))
        hi = sum(q_all[h, t, pl.ds(TOK, 8), :].astype(F32) for t in range(8, 16))
        both = jnp.concatenate([lo, hi], axis=1)
        masks.append(both[0:1])
        chosen.append(page_id.astype(F32) == both[1:2] * 32.0 + both[2:3])
        lse = top[h] + jnp.log(tot[h])
        value = masks[h] * (0.5 * (lse - log_count))
        total = select_dot(value, same[...])
        score[h] = total
        highest = jnp.max(total, axis=0, keepdims=True)
        lse_rows.append(highest + jnp.log(jnp.sum(jnp.exp(total - highest), axis=0, keepdims=True)))
        picked_rows.append(jnp.sum(jnp.where(chosen[h], total, 0.0), axis=0, keepdims=True))

    tok = jnp.bitwise_and(lane, 15)
    row = jnp.zeros((1, 128), F32)
    for j in range(4):
        part = slice(128 * (j % 2), 128 * (j % 2) + 128)
        piece = jnp.where(tok < 12, lse_rows[j // 2][:, part], picked_rows[j // 2][:, part])
        row = row + jnp.where(jnp.bitwise_and(tok, 3) == j, piece, 0.0)
    mine = c * NZ + z
    stat[mine] = row
    push(stat.at[mine], stat.at[mine], stat_sem.at[0], stat_sem.at[1], pair)
    for d in (8, 7, 9, 6, 10, 5, 11, 4, 12, 3, 13, 2, 14, 1, 15):
        for cc in (c, other):
            push(stat.at[mine], stat.at[mine], stat_sem.at[0], stat_sem.at[1], {"c": cc, **at_z(d)})
    order = []
    for r in (2, 1, 3, 0):
        for d in (2, 1, 3):
            order += [(4 * r + d, 0), (4 * d + r, 1)]
    order += [(4 * r, 0) for r in range(4)] + [(r, 1) for r in range(4)]
    phase("turn_pages")
    for i, (s, k) in enumerate(order):
        pages_t[:, pl.ds(128 * i, 128)] = pages[s, k].T
    phase("stat_wait")
    arrived(stat.at[pl.ds(0, 31)], stat_sem.at[1])
    phase("softmax")
    highest = stat[0]
    for d in range(1, 32):
        highest = jnp.maximum(highest, stat[d])
    total = jnp.zeros((1, 128), F32)
    picked = jnp.zeros((1, 128), F32)
    for d in range(32):
        total = total + jnp.exp(stat[d] - highest)
        picked = picked + stat[d]
    page_lse = highest + jnp.log(total)
    part = jnp.where(tok < 4, page_lse, jnp.where(tok >= 12, -picked, 0.0))
    column_loss = jnp.broadcast_to(jnp.sum(part, axis=1, keepdims=True), (1, 128))
    loss_x[x] = column_loss
    for d in (1, 2, 3):
        push(loss_x.at[x], loss_x.at[x], loss_sem.at[0], loss_sem.at[1], at_x(d))
    wide = select_dot(jnp.broadcast_to(page_lse, (8, 128)), spread[...])[0:1]
    for h in range(2):
        coefficient = jnp.exp(score[h] - wide[:, 256 * h : 256 * h + 256]) - jnp.where(chosen[h], 1.0, 0.0)
        coef[h] = coefficient * masks[h] / tot[h]

    phase("backward")
    queries = q_all[:, :, pl.ds(0, TOK), :].reshape(2 * ROWS, D)

    def form_factor(i):
        s, k = order[i]
        for h in range(2):
            value = e_all[h, s, k] * coef[h, pl.ds(2 * s + k, 1), :]
            factor[pl.ds(128 * i, 128), pl.ds(ROWS * h, ROWS)] = value.astype(BF16)

    def page_grads(start, stop):
        size = 2 if stop - start == 4 else 4
        for part in range(start, stop, size):
            grads = jnp.dot(factor[pl.ds(128 * part, 128 * size), :], queries, preferred_element_type=F32)
            for i in range(size):
                s, k = order[part + i]
                rx, ry = s // 4, s % 4
                g = grads[128 * i : 128 * i + 128]
                if (rx if k else ry) == 0:
                    (own_b if k else own_a)[ry if k else rx] = g
                else:
                    gp_send[s, k] = g.astype(BF16)
        for s, k in order[start:stop]:
            rx, ry = s // 4, s % 4
            if k == 0 and ry:
                push(gp_send.at[s, 0], mid_a.at[rx, 3 - ry], gp_send_sem, gp_recv.at[0, rx], at_y(ry))
            elif k == 1 and rx:
                push(gp_send.at[s, 1], mid_b.at[ry, 3 - rx], gp_send_sem, gp_recv.at[1, ry], at_x(rx))

    def query_grads():
        for h in range(2):
            gq_t[h] = jnp.dot(pages_t[...], factor[:, pl.ds(ROWS * h, ROWS)], preferred_element_type=F32)
        gq_pair[...] = gq_t[other].T
        push(gq_pair, gq_in, pair_send, pair_recv, pair)
        gq_own[...] = gq_t[c].T

    def query_grads_away():
        arrived(gq_in, pair_recv)
        gq_own[...] += gq_in[...]
        gq_send[...] = gq_own[...].astype(BF16).reshape(NZ, TOK, D)
        for d in (8, 7, 9, 6, 10, 5, 11, 4, 12, 3, 13, 2, 14, 1, 15):
            zz = lax.rem(z + d, NZ)
            push(gq_send.at[zz], gq_recv.at[z], gq_sem.at[0], gq_sem.at[1], at_z(d))

    def line_sum(r):
        arrived(mid_a.at[r], gp_recv.at[0, r])
        acc_a = own_a[r] + (mid_a[r, 0].astype(F32) + mid_a[r, 1].astype(F32) + mid_a[r, 2].astype(F32))
        if r:
            out_a[r - 1] = acc_a.astype(BF16)
            push(out_a.at[r - 1], in_a.at[3 - r], st2_send.at[0], st2_recv.at[0], at_x(r))
        else:
            own_a[0] = acc_a
        arrived(mid_b.at[r], gp_recv.at[1, r])
        acc_b = own_b[r] + (mid_b[r, 0].astype(F32) + mid_b[r, 1].astype(F32) + mid_b[r, 2].astype(F32))
        if r:
            out_b[r - 1] = acc_b.astype(BF16)
            push(out_b.at[r - 1], in_b.at[3 - r], st2_send.at[1], st2_recv.at[1], at_y(r))
        else:
            own_b[0] = acc_b

    def pass_loss():
        arrived(loss_x.at[pl.ds(0, 3)], loss_sem.at[1])
        line = loss_x[0] + loss_x[1] + loss_x[2] + loss_x[3]
        loss_y[y] = line
        for d in (1, 2, 3):
            push(loss_y.at[y], loss_y.at[y], loss_sem.at[2], loss_sem.at[3], at_y(d))

    @pl.when(z < 4)
    def _():
        for start, stop in ((0, 4), (4, 8), (8, 16), (16, 24), (24, 32)):
            for i in range(start, stop):
                form_factor(i)
            page_grads(start, stop)
        query_grads()
        pass_loss()
        line_sum(2)
        query_grads_away()

    @pl.when(z >= 4)
    def _():
        for i in range(32):
            form_factor(i)
        query_grads()
        page_grads(0, 8)
        page_grads(8, 16)
        query_grads_away()
        page_grads(16, 24)
        page_grads(24, 32)
        pass_loss()
        line_sum(2)

    phase("lines")
    line_sum(1)
    line_sum(3)
    phase("line_own")
    line_sum(0)

    phase("loss")
    arrived(loss_y.at[pl.ds(0, 3)], loss_sem.at[3])
    loss_ref[...] = (loss_y[0] + loss_y[1] + loss_y[2] + loss_y[3]) * (1.0 / 512.0)

    phase("gp_last")
    arrived(in_a, st2_recv.at[0])
    gp_ref[0] = own_a[0] + (in_a[0].astype(F32) + in_a[1].astype(F32) + in_a[2].astype(F32))
    arrived(in_b, st2_recv.at[1])
    gp_ref[1] = own_b[0] + (in_b[0].astype(F32) + in_b[1].astype(F32) + in_b[2].astype(F32))

    phase("gq_last")
    total = gq_own[pl.ds(pl.multiple_of(z * TOK, TOK), TOK), :]
    arrived(gq_recv.at[pl.ds(0, NZ - 1)], gq_sem.at[1])
    for d in range(1, NZ):
        zz = lax.rem(z + d, NZ)
        total = total + gq_recv[zz].astype(F32)
    gq_ref[0] = total

    phase("drain")
    arrived(q_all.at[c, pl.ds(0, NZ - 1)], q_send.at[0])
    arrived(q_all.at[c], q_send.at[1])
    arrived(pages.at[pl.ds(0, NS - 1)], pg_send)
    arrived(gq_pair, pair_send)
    arrived(stat.at[pl.ds(0, 31)], stat_sem.at[0])
    arrived(gp_send.at[pl.ds(0, 12)], gp_send_sem)
    arrived(out_a, st2_send.at[0])
    arrived(out_b, st2_send.at[1])
    arrived(gq_send.at[pl.ds(0, NZ - 1)], gq_sem.at[0])
    arrived(loss_x.at[pl.ds(0, 3)], loss_sem.at[0])
    arrived(loss_y.at[pl.ds(0, 3)], loss_sem.at[2])
    phase(None)


def write_out(gq_in, gp_in, loss_in, gq_hbm, gp_hbm, loss_hbm, loss_out, sem):
    loss_out[0] = loss_in[0, 0]
    copies = [
        pltpu.make_async_copy(gp_in, gp_hbm, sem.at[0]),
        pltpu.make_async_copy(gq_in, gq_hbm, sem.at[1]),
        pltpu.make_async_copy(loss_out, loss_hbm, sem.at[2]),
    ]
    for copy in copies:
        copy.start()
    for copy in copies:
        copy.wait()


def on_device(queries, query_mask, positive, page_vectors, page_mask):
    hbm = pl.BlockSpec(memory_space=pl.ANY)
    vmem = pl.BlockSpec(memory_space=pltpu.VMEM)
    V = pltpu.VMEM
    dma = pltpu.SemaphoreType.DMA
    scratch = [
        pltpu.SMEM((1, TOK), I32),
        pltpu.SMEM((1,), I32),
        V((2, 128, D), BF16),
        V((2, 128), I32),
        dma((5,)),
        V((2, NZ, TOK + 8, D), BF16),
        V((NS, 2, 128, D), BF16),
        V((D, NS * 256), BF16),
        V((2, 2 * D, ROWS), BF16),
        V((NS, 256, 128), BF16),
        V((ROWS, ROWS), BF16),
        V((128, 512), BF16),
        V((NS * 256, 2 * ROWS), BF16),
        V((2, NS, 2, 128, ROWS), F32),
        V((2, 32, ROWS), F32),
        V((2, 32, ROWS), F32),
        V((32, 128), F32),
        V((2, 32, ROWS), F32),
        V((2, 32, ROWS), F32),
        V((32, 1, 128), F32),
        V((2, D, ROWS), F32),
        V((NS, 2, 128, D), BF16),
        V((4, 128, D), F32),
        V((4, 128, D), F32),
        V((4, 3, 128, D), BF16),
        V((4, 3, 128, D), BF16),
        V((3, 128, D), BF16),
        V((3, 128, D), BF16),
        V((3, 128, D), BF16),
        V((3, 128, D), BF16),
        V((ROWS, D), F32),
        V((ROWS, D), F32),
        V((ROWS, D), F32),
        V((NZ, TOK, D), BF16),
        V((NZ, TOK, D), BF16),
        V((4, 1, 128), F32),
        V((4, 1, 128), F32),
        dma((2,)),
        dma((6,)),
        dma(()),
        dma(()),
        dma(()),
        dma((2, 3)),
        dma((2,)),
        dma((2,)),
        dma(()),
        dma((2, 4)),
        dma((2,)),
        dma((2,)),
        dma((2,)),
        dma((4,)),
    ]
    partial = pl.pallas_call(
        kernel,
        out_shape=(V((1, TOK, D), F32), V((2, 128, D), F32), V((1, 128), F32)),
        in_specs=[hbm, hbm, pl.BlockSpec(memory_space=pltpu.HBM), hbm, hbm],
        out_specs=(vmem, vmem, vmem),
        scratch_shapes=scratch,
        compiler_params=pltpu.CompilerParams(collective_id=0, has_side_effects=True),
    )(queries, query_mask, positive, page_vectors, page_mask)
    gq, gp, loss = pl.pallas_call(
        write_out,
        out_shape=(
            jax.ShapeDtypeStruct((1, TOK, D), F32),
            jax.ShapeDtypeStruct((2, 128, D), F32),
            jax.ShapeDtypeStruct((1,), F32),
        ),
        in_specs=[vmem] * 3,
        out_specs=(hbm, hbm, pl.BlockSpec(memory_space=pltpu.HBM)),
        scratch_shapes=[pltpu.SMEM((1,), F32), dma((3,))],
        compiler_params=pltpu.CompilerParams(vmem_limit_bytes=1 << 20),
    )(*[pltpu.with_memory_space_constraint(p, pltpu.VMEM) for p in partial])
    return gq, gp, loss.reshape(())


def solution(mesh):
    split = Mesh(mesh.devices.reshape(2, 4, 2, 2, 16), AXES)
    return jax.shard_map(
        on_device,
        mesh=split,
        in_specs=(P(AXES, None, None), P(AXES, None), P(AXES), P(AXES, None, None), P(AXES, None)),
        out_specs=(P(AXES, None, None), P(AXES, None, None), P()),
        check_vma=False,
    )
```

```python
import math

import jax
import jax.numpy as jnp
from jax import lax
from jax.experimental import pallas as pl
from jax.experimental.pallas import tpu as pltpu
from jax.sharding import Mesh
from jax.sharding import PartitionSpec as P

AXES = ("xl", "y", "c", "xh", "z")
MESH = pl.DeviceIdType.MESH
F32, BF16, I32 = jnp.float32, jnp.bfloat16, jnp.int32
NZ = 16
NS = 16
TOK = 16
D = 128
ROWS = NZ * TOK
STEP = 4
FLOOR = -1e30
RATE = 2.0 * math.log2(math.e)
MARK = 128.0


def iota(shape, dim):
    return lax.broadcasted_iota(I32, shape, dim)


def select_dot(a, chooser):
    parts, rest = [], a
    for _ in range(3):
        parts.append(rest.astype(BF16))
        rest = rest - parts[-1].astype(F32)
    n = a.shape[0]
    out = jnp.dot(jnp.concatenate(parts, axis=0), chooser, preferred_element_type=F32)
    return out[:n] + out[n : 2 * n] + out[2 * n :]


def kernel(
    q_hbm,
    qmask_hbm,
    pos_hbm,
    pg_hbm,
    pmask_hbm,
    gq_ref,
    gp_ref,
    loss_ref,
    qmask,
    pos,
    pg_in,
    pmask,
    load_sem,
    q_all,
    pages,
    pages_t,
    q_t,
    bias,
    same,
    spread,
    factor,
    e_all,
    top,
    tot,
    logn,
    score,
    coef,
    stat,
    gq_t,
    gp_send,
    own_a,
    own_b,
    mid_a,
    mid_b,
    out_a,
    out_b,
    in_a,
    in_b,
    gq_pair,
    gq_in,
    gq_own,
    gq_send,
    gq_recv,
    loss_x,
    loss_y,
    q_send,
    q_recv,
    pair_send,
    pair_recv,
    pg_send,
    line_recv,
    far_recv,
    stat_sem,
    gp_send_sem,
    gp_recv,
    st2_send,
    st2_recv,
    gq_sem,
    loss_sem,
):
    xl, y, c, xh, z = (lax.axis_index(a) for a in AXES)
    x = xh * 2 + xl
    other = 1 - c

    def at_x(d):
        t = lax.rem(x + d, 4)
        return {"xl": lax.rem(t, 2), "xh": lax.div(t, 2)}

    def at_y(d):
        return {"y": lax.rem(y + d, 4)}

    def at_z(d):
        return {"z": lax.rem(z + d, NZ)}

    pair = {"c": other}

    scopes = []

    def phase(name):
        if scopes:
            scopes.pop().__exit__(None, None, None)
        if name:
            scopes.append(jax.named_scope(name))
            scopes[-1].__enter__()

    def push(src, dst, ssem, rsem, device):
        copy = pltpu.make_async_remote_copy(
            src_ref=src, dst_ref=dst, send_sem=ssem, recv_sem=rsem, device_id=device, device_id_type=MESH
        )
        copy.start()

    def arrived(ref, sem):
        pltpu.make_async_copy(ref, ref, sem).wait()

    phase("entry")
    barrier = pltpu.get_barrier_semaphore()
    near = [s for d in range(1, STEP + 1) for s in (d, NZ - d)]
    peers = [at_z(d) for d in near] + [pair] + [at_x(d) for d in (1, 2, 3)] + [at_y(d) for d in (1, 2, 3)]
    for device in peers:
        pl.semaphore_signal(barrier, inc=1, device_id=device, device_id_type=MESH)

    phase("own")
    loads = [
        pltpu.make_async_copy(pg_hbm, pg_in, load_sem.at[0]),
        pltpu.make_async_copy(pmask_hbm, pmask, load_sem.at[1]),
        pltpu.make_async_copy(q_hbm.at[0], q_all.at[c, z, pl.ds(0, TOK)], load_sem.at[2]),
        pltpu.make_async_copy(qmask_hbm, qmask, load_sem.at[3]),
        pltpu.make_async_copy(pos_hbm, pos, load_sem.at[4]),
    ]
    for load in loads:
        load.start()
    krow = iota((D, ROWS), 0)
    for h in range(2):
        q_t[h, pl.ds(D, D), :] = jnp.where(krow == 0, 1.0, 0.0).astype(BF16)
    together = lax.shift_right_logical(iota((ROWS, ROWS), 0), 4) == lax.shift_right_logical(iota((ROWS, ROWS), 1), 4)
    same[...] = jnp.where(together, 1.0, 0.0).astype(BF16)
    lane_out = iota((128, 512), 1)
    source = jnp.bitwise_and(lane_out, 112) + lax.shift_right_logical(lane_out, 7)
    spread[...] = jnp.where(iota((128, 512), 0) == source, 1.0, 0.0).astype(BF16)
    for load in loads:
        load.wait()
    prow = iota((128, 128), 0)
    for k in range(2):
        count = jnp.sum(pmask[pl.ds(k, 1), :].astype(F32), axis=1, keepdims=True)
        keep = jnp.logical_or(prow < 127, jnp.broadcast_to(count, (128, 128)) > 127.5)
        pages[0, k] = jnp.where(keep, pg_in[k].astype(F32), MARK + count).astype(BF16)
    lane = iota((1, 128), 1)
    base = lax.rem(z, 8) * TOK
    mask = jnp.zeros((1, 128), I32)
    for t in range(TOK):
        mask = mask + jnp.where(lane == base + t, qmask[0, t], 0)
    group = lax.shift_right_logical(lane, 4) == lax.rem(z, 8)
    page_hi = jnp.where(group, lax.shift_right_logical(pos[0], 5), 0)
    page_lo = jnp.where(group, jnp.bitwise_and(pos[0], 31), 0)
    mrow = iota((8, 128), 0)
    meta = jnp.where(mrow == 0, mask, jnp.where(mrow == 1, page_hi, jnp.where(mrow == 2, page_lo, 0)))
    q_all[c, z, pl.ds(TOK, 8), :] = meta.astype(F32).astype(BF16)

    phase("barrier")
    pl.semaphore_wait(barrier, len(peers))

    phase("issue")

    for d in reversed(near):
        sem = q_recv.at[0 if d == STEP else 1 if d == NZ - STEP else 2]
        push(q_all.at[c, z], q_all.at[c, z], q_send.at[0], sem, at_z(d))

    def pass_query(zsrc, d):
        push(q_all.at[c, zsrc], q_all.at[c, zsrc], q_send.at[0], q_recv.at[3], at_z(d))
        push(q_all.at[c, zsrc], q_all.at[c, zsrc], q_send.at[1], q_recv.at[5], {"c": other, **at_z(d)})

    for d in (2, 1, 3):
        push(pages.at[0, 0], pages.at[4 * (4 - d), 0], pg_send, line_recv.at[0, d - 1], at_x(d))
        push(pages.at[0, 1], pages.at[4 - d, 1], pg_send, line_recv.at[1, d - 1], at_y(d))
    for d in (2, 1, 3):
        push(pages.at[0, 1], pages.at[4 * (4 - d), 1], pg_send, far_recv.at[0], at_x(d))
        push(pages.at[0, 0], pages.at[4 - d, 0], pg_send, far_recv.at[0], at_y(d))

    def relay(d):
        arrived(pages.at[4 * d, 0], line_recv.at[0, 3 - d])
        for e in (2, 1, 3):
            push(pages.at[4 * d, 0], pages.at[4 * d + 4 - e, 0], pg_send, far_recv.at[1], at_y(e))
        arrived(pages.at[d, 1], line_recv.at[1, 3 - d])
        for e in (2, 1, 3):
            push(pages.at[d, 1], pages.at[4 * (4 - e) + d, 1], pg_send, far_recv.at[1], at_x(e))

    phase("relay")
    relay(1)
    relay(3)
    phase("query_near")
    arrived(q_all.at[c, pl.ds(0, 6)], q_recv.at[2])
    behind, ahead = lax.rem(z + NZ - STEP, NZ), lax.rem(z + STEP, NZ)
    arrived(q_all.at[c, behind], q_recv.at[0])
    arrived(q_all.at[c, ahead], q_recv.at[1])
    for d in range(STEP, 0, -1):
        pass_query(behind, d)
    for d in range(STEP - 1, 0, -1):
        pass_query(ahead, NZ - d)
    for d in [0] + near:
        zsrc = lax.rem(z + d, NZ)
        push(q_all.at[c, zsrc], q_all.at[c, zsrc], q_send.at[1], q_recv.at[4], pair)
    phase("relay_2")
    relay(2)

    def turn_queries(h):
        q_t[h, pl.ds(0, D), :] = q_all[h, :, pl.ds(0, TOK), :].reshape(ROWS, D).T

    first = iota((128, 128), 1) == 0

    def count_patches(slots):
        for rx, ry in slots:
            s = 4 * rx + ry
            for k in range(2):
                last = pages[s, k, pl.ds(112, 16), :].astype(F32)[15:16]
                count = jnp.where(last > 100.0, last - MARK, 128.0)
                logn[pl.ds(2 * s + k, 1), :] = count
                unused = jnp.logical_and(first, prow >= jnp.broadcast_to(count.astype(I32), (128, 128)))
                bias[s, pl.ds(128 * k, 128), :] = jnp.where(unused, FLOOR, 0.0).astype(BF16)

    def forward(h, slots):
        for rx, ry in slots:
            s = 4 * rx + ry
            block = jnp.concatenate([pages[s].reshape(256, D), bias[s]], axis=1)
            dots = jnp.dot(block, q_t[h], preferred_element_type=F32)
            for k in range(2):
                row = pl.ds(2 * s + k, 1)
                for v in range(2):
                    lanes = pl.ds(128 * v, 128)
                    part = dots[128 * k : 128 * k + 128, 128 * v : 128 * v + 128]
                    highest = jnp.max(part, axis=0, keepdims=True)
                    e = jnp.exp2((part - highest) * RATE)
                    e_all[h, s, k, :, lanes] = e
                    top[h, row, lanes] = highest * 2.0
                    tot[h, row, lanes] = jnp.sum(e, axis=0, keepdims=True)

    line_slots = [(0, 0), (1, 0), (0, 1), (3, 0), (0, 3), (2, 0), (0, 2)]
    far_slots = [(dx, dy) for dx in (1, 3, 2) for dy in (1, 3, 2)]
    arrived(pages.at[pl.ds(0, 3)], far_recv.at[0])
    count_patches(line_slots)
    def own_far():
        arrived(q_all.at[c, pl.ds(0, 7)], q_recv.at[3])

    def other_core():
        arrived(q_all.at[other, pl.ds(0, 9)], q_recv.at[4])
        arrived(q_all.at[other, pl.ds(0, 7)], q_recv.at[5])

    phase("query_far")
    pl.when(c == 1)(own_far)
    pl.when(c == 0)(other_core)
    phase("forward_1")
    turn_queries(1)
    forward(1, line_slots)
    phase("pages_far")
    arrived(pages.at[pl.ds(0, 9)], far_recv.at[1])
    phase("forward_far")
    count_patches(far_slots)
    forward(1, far_slots)
    phase("query_pair")
    pl.when(c == 0)(own_far)
    pl.when(c == 1)(other_core)
    phase("forward_0")
    turn_queries(0)
    forward(0, line_slots + far_slots)

    phase("scores")
    i = iota((32, ROWS), 0)
    px = jnp.bitwise_and(x + lax.shift_right_logical(i, 3), 3)
    py = jnp.bitwise_and(y + jnp.bitwise_and(lax.shift_right_logical(i, 1), 3), 3)
    blk = (jnp.bitwise_and(px, 1) * 4 + py) * 2 + c
    page_id = (blk * 32 + lax.shift_right_logical(px, 1) * 16 + z) * 2 + jnp.bitwise_and(i, 1)
    log_count = jnp.log(logn[...])
    log_count = jnp.concatenate([log_count, log_count], axis=1)
    masks, chosen, lse_rows, picked_rows = [], [], [], []
    values = []
    for h in range(2):
        lo = sum(q_all[h, t, pl.ds(TOK, 8), :].astype(F32) for t in range(8))
        hi = sum(q_all[h, t, pl.ds(TOK, 8), :].astype(F32) for t in range(8, 16))
        both = jnp.concatenate([lo, hi], axis=1)
        masks.append(both[0:1])
        chosen.append(page_id.astype(F32) == both[1:2] * 32.0 + both[2:3])
        lse = top[h] + jnp.log(tot[h])
        values.append(masks[h] * (0.5 * (lse - log_count)))
    totals = select_dot(jnp.concatenate(values, axis=0), same[...])
    for h in range(2):
        total = totals[32 * h : 32 * h + 32]
        score[h] = total
        highest = jnp.max(total, axis=0, keepdims=True)
        lse_rows.append(highest + jnp.log(jnp.sum(jnp.exp(total - highest), axis=0, keepdims=True)))
        picked_rows.append(jnp.sum(jnp.where(chosen[h], total, 0.0), axis=0, keepdims=True))

    tok = jnp.bitwise_and(lane, 15)
    row = jnp.zeros((1, 128), F32)
    for j in range(4):
        part = slice(128 * (j % 2), 128 * (j % 2) + 128)
        piece = jnp.where(tok < 12, lse_rows[j // 2][:, part], picked_rows[j // 2][:, part])
        row = row + jnp.where(jnp.bitwise_and(tok, 3) == j, piece, 0.0)
    mine = c * NZ + z
    stat[mine] = row
    push(stat.at[mine], stat.at[mine], stat_sem.at[0], stat_sem.at[1], pair)
    for d in (8, 7, 9, 6, 10, 5, 11, 4, 12, 3, 13, 2, 14, 1, 15):
        for cc in (c, other):
            push(stat.at[mine], stat.at[mine], stat_sem.at[0], stat_sem.at[1], {"c": cc, **at_z(d)})
    order = []
    for r in (2, 1, 3, 0):
        for d in (2, 1, 3):
            order += [(4 * r + d, 0), (4 * d + r, 1)]
    order += [(4 * r, 0) for r in range(4)] + [(r, 1) for r in range(4)]
    phase("turn_pages")
    for i, (s, k) in enumerate(order):
        pages_t[:, pl.ds(128 * i, 128)] = pages[s, k].T
    phase("stat_wait")
    arrived(stat.at[pl.ds(0, 31)], stat_sem.at[1])
    phase("softmax")
    highest = stat[0]
    for d in range(1, 32):
        highest = jnp.maximum(highest, stat[d])
    total = jnp.zeros((1, 128), F32)
    picked = jnp.zeros((1, 128), F32)
    for d in range(32):
        total = total + jnp.exp(stat[d] - highest)
        picked = picked + stat[d]
    page_lse = highest + jnp.log(total)
    part = jnp.where(tok < 4, page_lse, jnp.where(tok >= 12, -picked, 0.0))
    column_loss = jnp.broadcast_to(jnp.sum(part, axis=1, keepdims=True), (1, 128))
    loss_x[x] = column_loss
    for d in (1, 2, 3):
        push(loss_x.at[x], loss_x.at[x], loss_sem.at[0], loss_sem.at[1], at_x(d))
    wide = select_dot(jnp.broadcast_to(page_lse, (8, 128)), spread[...])[0:1]
    for h in range(2):
        coefficient = jnp.exp(score[h] - wide[:, 256 * h : 256 * h + 256]) - jnp.where(chosen[h], 1.0, 0.0)
        coef[h] = coefficient * masks[h] / tot[h]

    phase("backward")
    queries = q_all[:, :, pl.ds(0, TOK), :].reshape(2 * ROWS, D)

    def form_factor(i):
        s, k = order[i]
        for h in range(2):
            value = e_all[h, s, k] * coef[h, pl.ds(2 * s + k, 1), :]
            factor[pl.ds(128 * i, 128), pl.ds(ROWS * h, ROWS)] = value.astype(BF16)

    def page_grads(start, stop):
        size = 2 if stop - start == 4 else 4
        for part in range(start, stop, size):
            grads = jnp.dot(factor[pl.ds(128 * part, 128 * size), :], queries, preferred_element_type=F32)
            for i in range(size):
                s, k = order[part + i]
                rx, ry = s // 4, s % 4
                g = grads[128 * i : 128 * i + 128]
                if (rx if k else ry) == 0:
                    (own_b if k else own_a)[ry if k else rx] = g
                else:
                    gp_send[s, k] = g.astype(BF16)
        for s, k in order[start:stop]:
            rx, ry = s // 4, s % 4
            if k == 0 and ry:
                push(gp_send.at[s, 0], mid_a.at[rx, 3 - ry], gp_send_sem, gp_recv.at[0, rx], at_y(ry))
            elif k == 1 and rx:
                push(gp_send.at[s, 1], mid_b.at[ry, 3 - rx], gp_send_sem, gp_recv.at[1, ry], at_x(rx))

    def query_grads():
        for h in range(2):
            gq_t[h] = jnp.dot(pages_t[...], factor[:, pl.ds(ROWS * h, ROWS)], preferred_element_type=F32)
        gq_pair[...] = gq_t[other].T
        push(gq_pair, gq_in, pair_send, pair_recv, pair)
        gq_own[...] = gq_t[c].T

    def query_grads_away():
        arrived(gq_in, pair_recv)
        gq_own[...] += gq_in[...]
        gq_send[...] = gq_own[...].astype(BF16).reshape(NZ, TOK, D)
        for d in (8, 7, 9, 6, 10, 5, 11, 4, 12, 3, 13, 2, 14, 1, 15):
            zz = lax.rem(z + d, NZ)
            push(gq_send.at[zz], gq_recv.at[z], gq_sem.at[0], gq_sem.at[1], at_z(d))

    def line_sum(r):
        arrived(mid_a.at[r], gp_recv.at[0, r])
        acc_a = own_a[r] + (mid_a[r, 0].astype(F32) + mid_a[r, 1].astype(F32) + mid_a[r, 2].astype(F32))
        if r:
            out_a[r - 1] = acc_a.astype(BF16)
            push(out_a.at[r - 1], in_a.at[3 - r], st2_send.at[0], st2_recv.at[0], at_x(r))
        else:
            own_a[0] = acc_a
        arrived(mid_b.at[r], gp_recv.at[1, r])
        acc_b = own_b[r] + (mid_b[r, 0].astype(F32) + mid_b[r, 1].astype(F32) + mid_b[r, 2].astype(F32))
        if r:
            out_b[r - 1] = acc_b.astype(BF16)
            push(out_b.at[r - 1], in_b.at[3 - r], st2_send.at[1], st2_recv.at[1], at_y(r))
        else:
            own_b[0] = acc_b

    def pass_loss():
        arrived(loss_x.at[pl.ds(0, 3)], loss_sem.at[1])
        line = loss_x[0] + loss_x[1] + loss_x[2] + loss_x[3]
        loss_y[y] = line
        for d in (1, 2, 3):
            push(loss_y.at[y], loss_y.at[y], loss_sem.at[2], loss_sem.at[3], at_y(d))

    @pl.when(z < 4)
    def _():
        for start, stop in ((0, 4), (4, 8), (8, 16), (16, 24), (24, 32)):
            for i in range(start, stop):
                form_factor(i)
            page_grads(start, stop)
        query_grads()
        pass_loss()
        line_sum(2)
        query_grads_away()

    @pl.when(z >= 4)
    def _():
        for i in range(32):
            form_factor(i)
        query_grads()
        page_grads(0, 8)
        page_grads(8, 16)
        query_grads_away()
        page_grads(16, 24)
        page_grads(24, 32)
        pass_loss()
        line_sum(2)

    phase("lines")
    line_sum(1)
    line_sum(3)
    phase("line_own")
    line_sum(0)

    phase("loss")
    arrived(loss_y.at[pl.ds(0, 3)], loss_sem.at[3])
    loss_ref[...] = (loss_y[0] + loss_y[1] + loss_y[2] + loss_y[3]) * (1.0 / 512.0)

    phase("gp_last")
    arrived(in_a, st2_recv.at[0])
    gp_ref[0] = own_a[0] + (in_a[0].astype(F32) + in_a[1].astype(F32) + in_a[2].astype(F32))
    arrived(in_b, st2_recv.at[1])
    gp_ref[1] = own_b[0] + (in_b[0].astype(F32) + in_b[1].astype(F32) + in_b[2].astype(F32))

    phase("gq_last")
    total = gq_own[pl.ds(pl.multiple_of(z * TOK, TOK), TOK), :]
    arrived(gq_recv.at[pl.ds(0, NZ - 1)], gq_sem.at[1])
    for d in range(1, NZ):
        zz = lax.rem(z + d, NZ)
        total = total + gq_recv[zz].astype(F32)
    gq_ref[0] = total

    phase("drain")
    arrived(q_all.at[c, pl.ds(0, NZ - 1)], q_send.at[0])
    arrived(q_all.at[c], q_send.at[1])
    arrived(pages.at[pl.ds(0, NS - 1)], pg_send)
    arrived(gq_pair, pair_send)
    arrived(stat.at[pl.ds(0, 31)], stat_sem.at[0])
    arrived(gp_send.at[pl.ds(0, 12)], gp_send_sem)
    arrived(out_a, st2_send.at[0])
    arrived(out_b, st2_send.at[1])
    arrived(gq_send.at[pl.ds(0, NZ - 1)], gq_sem.at[0])
    arrived(loss_x.at[pl.ds(0, 3)], loss_sem.at[0])
    arrived(loss_y.at[pl.ds(0, 3)], loss_sem.at[2])
    phase(None)


def write_out(gq_in, gp_in, loss_in, gq_hbm, gp_hbm, loss_hbm, loss_out, sem):
    loss_out[0] = loss_in[0, 0]
    copies = [
        pltpu.make_async_copy(gp_in, gp_hbm, sem.at[0]),
        pltpu.make_async_copy(gq_in, gq_hbm, sem.at[1]),
        pltpu.make_async_copy(loss_out, loss_hbm, sem.at[2]),
    ]
    for copy in copies:
        copy.start()
    for copy in copies:
        copy.wait()


def on_device(queries, query_mask, positive, page_vectors, page_mask):
    hbm = pl.BlockSpec(memory_space=pl.ANY)
    vmem = pl.BlockSpec(memory_space=pltpu.VMEM)
    V = pltpu.VMEM
    dma = pltpu.SemaphoreType.DMA
    scratch = [
        pltpu.SMEM((1, TOK), I32),
        pltpu.SMEM((1,), I32),
        V((2, 128, D), BF16),
        V((2, 128), I32),
        dma((5,)),
        V((2, NZ, TOK + 8, D), BF16),
        V((NS, 2, 128, D), BF16),
        V((D, NS * 256), BF16),
        V((2, 2 * D, ROWS), BF16),
        V((NS, 256, 128), BF16),
        V((ROWS, ROWS), BF16),
        V((128, 512), BF16),
        V((NS * 256, 2 * ROWS), BF16),
        V((2, NS, 2, 128, ROWS), F32),
        V((2, 32, ROWS), F32),
        V((2, 32, ROWS), F32),
        V((32, 128), F32),
        V((2, 32, ROWS), F32),
        V((2, 32, ROWS), F32),
        V((32, 1, 128), F32),
        V((2, D, ROWS), F32),
        V((NS, 2, 128, D), BF16),
        V((4, 128, D), F32),
        V((4, 128, D), F32),
        V((4, 3, 128, D), BF16),
        V((4, 3, 128, D), BF16),
        V((3, 128, D), BF16),
        V((3, 128, D), BF16),
        V((3, 128, D), BF16),
        V((3, 128, D), BF16),
        V((ROWS, D), F32),
        V((ROWS, D), F32),
        V((ROWS, D), F32),
        V((NZ, TOK, D), BF16),
        V((NZ, TOK, D), BF16),
        V((4, 1, 128), F32),
        V((4, 1, 128), F32),
        dma((2,)),
        dma((6,)),
        dma(()),
        dma(()),
        dma(()),
        dma((2, 3)),
        dma((2,)),
        dma((2,)),
        dma(()),
        dma((2, 4)),
        dma((2,)),
        dma((2,)),
        dma((2,)),
        dma((4,)),
    ]
    partial = pl.pallas_call(
        kernel,
        out_shape=(V((1, TOK, D), F32), V((2, 128, D), F32), V((1, 128), F32)),
        in_specs=[hbm, hbm, pl.BlockSpec(memory_space=pltpu.HBM), hbm, hbm],
        out_specs=(vmem, vmem, vmem),
        scratch_shapes=scratch,
        compiler_params=pltpu.CompilerParams(collective_id=0, has_side_effects=True),
    )(queries, query_mask, positive, page_vectors, page_mask)
    gq, gp, loss = pl.pallas_call(
        write_out,
        out_shape=(
            jax.ShapeDtypeStruct((1, TOK, D), F32),
            jax.ShapeDtypeStruct((2, 128, D), F32),
            jax.ShapeDtypeStruct((1,), F32),
        ),
        in_specs=[vmem] * 3,
        out_specs=(hbm, hbm, pl.BlockSpec(memory_space=pltpu.HBM)),
        scratch_shapes=[pltpu.SMEM((1,), F32), dma((3,))],
        compiler_params=pltpu.CompilerParams(vmem_limit_bytes=1 << 20),
    )(*[pltpu.with_memory_space_constraint(p, pltpu.VMEM) for p in partial])
    return gq, gp, loss.reshape(())


def solution(mesh):
    split = Mesh(mesh.devices.reshape(2, 4, 2, 2, 16), AXES)
    return jax.shard_map(
        on_device,
        mesh=split,
        in_specs=(P(AXES, None, None), P(AXES, None), P(AXES), P(AXES, None, None), P(AXES, None)),
        out_specs=(P(AXES, None, None), P(AXES, None, None), P()),
        check_vma=False,
    )
```
